16 devices in a mesh: col: 4 (over z, y), row: 4 (over x, core).
Axes of the slice: x: 2, y: 2, z: 2, core: 2. Of those that a mesh axis runs over, the one named last changes fastest.
Arguments:
- image: bfloat16 [1, 512, 512, 128], P(None, 'row', 'col')
- w_first: bfloat16 [3, 3, 128, 128], replicated
- w_second: bfloat16 [3, 3, 128, 128], replicated
- w_third: bfloat16 [3, 3, 128, 128], replicated
- grad_out: bfloat16 [1, 512, 512, 128], P(None, 'row', 'col')
Outputs:
- output 1: bfloat16 [1, 512, 512, 128], P(None, 'row', 'col')
- output 2: bfloat16 [1, 512, 512, 128], P(None, 'row', 'col')
- output 3: float32 [3, 3, 128, 128], replicated
- output 4: float32 [3, 3, 128, 128], replicated
- output 5: float32 [3, 3, 128, 128], replicated
All inputs are finite; a program needn't handle non-finite values.
Results may differ from the reference program's by a relative error of at most 0.0141409.
Values are sent between devices in bfloat16 or wider.
A program may use at most 1 GiB of HBM per device.

```python
import math
import jax
import jax.numpy as jnp
from jax import lax

IMG_BATCH = 1
IMG_HEIGHT = 512
IMG_WIDTH = 512
CHANNELS = 128

GELU_SCALE = math.sqrt(2.0 / math.pi)
GELU_CUBIC = 0.044715
SAME_PAD = ((1, 1), (1, 1))


def gelu_tanh(value):
    return 0.5 * value * (1.0 + jnp.tanh(GELU_SCALE * (value + GELU_CUBIC * value * value * value)))


def gelu_slope(value):
    tanh_val = jnp.tanh(GELU_SCALE * (value + GELU_CUBIC * value * value * value))
    return 0.5 * (1.0 + tanh_val) + 0.5 * value * (1.0 - tanh_val * tanh_val) * GELU_SCALE * (1.0 + 3.0 * GELU_CUBIC * value * value)


def conv_same(values, weight):
    return lax.conv_general_dilated(values.astype(jnp.float32), weight.astype(jnp.float32), (1, 1), SAME_PAD, dimension_numbers=('NHWC', 'HWIO', 'NHWC'))


def conv_transpose(grad, weight):
    return lax.conv_general_dilated(grad.astype(jnp.float32), lax.rev(weight, (0, 1)).astype(jnp.float32), (1, 1), SAME_PAD, dimension_numbers=('NHWC', 'HWOI', 'NHWC'))


def weight_grad(values, grad):
    padded = jnp.pad(values.astype(jnp.float32), ((0, 0), (1, 1), (1, 1), (0, 0)))
    return lax.conv_general_dilated(padded, grad.astype(jnp.float32), (1, 1), 'VALID', dimension_numbers=('CHWN', 'IHWO', 'HWNC'))


def setup_inputs(seed: int = 0) -> dict:
    key = jax.random.key(seed)
    k_img, k_one, k_two, k_three, k_grad = jax.random.split(key, 5)
    act_shape = (IMG_BATCH, IMG_HEIGHT, IMG_WIDTH, CHANNELS)
    w_shape = (3, 3, CHANNELS, CHANNELS)
    fan_scale = (9 * CHANNELS) ** -0.5
    image = jax.random.normal(k_img, act_shape, jnp.float32).astype(jnp.bfloat16)
    w_first = (jax.random.normal(k_one, w_shape, jnp.float32) * fan_scale).astype(jnp.bfloat16)
    w_second = (jax.random.normal(k_two, w_shape, jnp.float32) * fan_scale).astype(jnp.bfloat16)
    w_third = (jax.random.normal(k_three, w_shape, jnp.float32) * fan_scale).astype(jnp.bfloat16)
    grad_out = jax.random.normal(k_grad, act_shape, jnp.float32).astype(jnp.bfloat16)
    return {'image': image, 'w_first': w_first, 'w_second': w_second, 'w_third': w_third, 'grad_out': grad_out}


def reference(image, w_first, w_second, w_third, grad_out):
    pre_one = conv_same(image, w_first).astype(jnp.bfloat16)
    act_one = gelu_tanh(pre_one.astype(jnp.float32)).astype(jnp.bfloat16)
    pre_two = conv_same(act_one, w_second).astype(jnp.bfloat16)
    act_two = gelu_tanh(pre_two.astype(jnp.float32)).astype(jnp.bfloat16)
    block_out = (conv_same(act_two, w_third) + image.astype(jnp.float32)).astype(jnp.bfloat16)
    grad_pre2 = (conv_transpose(grad_out, w_third) * gelu_slope(pre_two.astype(jnp.float32))).astype(jnp.bfloat16)
    grad_pre1 = (conv_transpose(grad_pre2, w_second) * gelu_slope(pre_one.astype(jnp.float32))).astype(jnp.bfloat16)
    grad_image = (conv_transpose(grad_pre1, w_first) + grad_out.astype(jnp.float32)).astype(jnp.bfloat16)
    grad_w_first = weight_grad(image, grad_pre1)
    grad_w_second = weight_grad(act_one, grad_pre2)
    grad_w_third = weight_grad(act_two, grad_out)
    return (block_out, grad_image, grad_w_first, grad_w_second, grad_w_third)
```

```python
import functools
import math
import jax
import jax.numpy as jnp
from jax import lax
from jax.experimental import pallas as pl
from jax.experimental.pallas import tpu as pltpu
from jax.sharding import PartitionSpec as P

GELU_SCALE = math.sqrt(2.0 / math.pi)
GELU_CUBIC = 0.044715
BF16 = jnp.bfloat16
F32 = jnp.float32

TILE = 128
CH = 128
ROW_HALO = 4
COL_HALO = 8
STRIPS = 16
STEPS = 9
PAD_STEPS = STEPS + 2
PAIRS = 68
FIRST_OWN = ROW_HALO // 2
OWN_PAIRS = TILE // 2
EXT_ROWS = TILE + 2 * ROW_HALO
EXT_COLS = TILE + 2 * COL_HALO
STAGE_ROWS = 8


def gelu_tanh(value):
    return 0.5 * value * (1.0 + jnp.tanh(GELU_SCALE * (value + GELU_CUBIC * value * value * value)))


def gelu_slope(value):
    tanh_val = jnp.tanh(GELU_SCALE * (value + GELU_CUBIC * value * value * value))
    return 0.5 * (1.0 + tanh_val) + 0.5 * value * (1.0 - tanh_val * tanh_val) * GELU_SCALE * (1.0 + 3.0 * GELU_CUBIC * value * value)


def row_at(ref, k, r, off):
    pair = k - 1 if r == 0 else k + 1 if r == 3 else k
    return pair + off, (r + 1) % 2


def pack_weights(w_ref, wp_ref, back):
    zero = jnp.zeros((CH, CH), BF16)
    for q in range(3):
        for p in range(3):
            if back:
                block = w_ref[2 - p, 2 - q].astype(F32).T.astype(BF16)
            else:
                block = w_ref[p, q]
            for b in range(2):
                wp_ref[pl.ds((q * 4 + p + b) * CH, CH), pl.ds(b * CH, CH)] = block
        wp_ref[pl.ds((q * 4 + 3) * CH, CH), pl.ds(0, CH)] = zero
        wp_ref[pl.ds((q * 4) * CH, CH), pl.ds(CH, CH)] = zero


def conv_stage(src, off, wp, first, count, per_step, epilogue):
    def body(step, carry):
        base = first + step * per_step
        for j in range(per_step):
            k = base + j
            parts = []
            for q in range(3):
                for r in range(4):
                    pair, par = row_at(src, k, r, off)
                    parts.append(src[pair, par, q:q + STEPS].reshape(STEPS * STRIPS, CH))
            acc = jnp.dot(jnp.concatenate(parts, axis=1), wp[...], preferred_element_type=F32)
            for par in range(2):
                epilogue(k, par, j, acc[:, par * CH:(par + 1) * CH].reshape(STEPS, STRIPS, CH))
        return carry
    lax.fori_loop(0, count // per_step, body, 0)


def with_edges(value):
    left = pltpu.roll(value[STEPS - 1], 1, 0)[None]
    right = pltpu.roll(value[0], STRIPS - 1, 0)[None]
    return jnp.concatenate([left, value, right], axis=0)


def wgrad_stage(val, off, grad, own_mask, acc, out, per_step):
    dims = (((0,), (0,)), ((), ()))
    flat = per_step * STEPS * STRIPS
    acc[...] = jnp.zeros_like(acc)

    def rows_of(k, r):
        pair, par = row_at(val, k, r, off)
        return val[pl.ds(pair, per_step), par, 1:1 + STEPS].reshape(flat, CH)

    def body(step, carry):
        k = FIRST_OWN + step * per_step
        rows = [rows_of(k, r) for r in range(4)]
        shifted = []
        for par in range(2):
            d = grad[pl.ds(k, per_step), par] * own_mask[...][None]
            shifted.append([d[:, 2 - q:2 - q + STEPS].reshape(flat, CH) for q in range(3)])
        lhs = jnp.concatenate([jnp.concatenate(rows[par:par + 3], axis=1) for par in range(2)], axis=0)
        rhs = jnp.concatenate([jnp.concatenate(shifted[par][:2], axis=1) for par in range(2)], axis=0)
        acc[:, 0:2 * CH] += lax.dot_general(lhs, rhs, dims, preferred_element_type=F32)
        both = jnp.concatenate([shifted[0][2], shifted[1][2]], axis=1)
        last = lax.dot_general(jnp.concatenate(rows, axis=1), both, dims, preferred_element_type=F32)
        acc[:, 2 * CH:3 * CH] += last[0:3 * CH, 0:CH] + last[CH:4 * CH, CH:2 * CH]
        return carry

    lax.fori_loop(0, OWN_PAIRS // per_step, body, 0)
    for p in range(3):
        for q in range(3):
            out[p, q] = acc[p * CH:(p + 1) * CH, q * CH:(q + 1) * CH]


def block_kernel(image, grad, w_first, w_second, w_third,
                 block_out, grad_image, dw_first, dw_second, dw_third,
                 xp, one, two, gp, d_two, d_one, a_one, a_two, wp,
                 stage, wide, outs, acc, img_mask, own_mask, in_sems, out_sems):
    row_id = lax.axis_index('row')
    col_id = lax.axis_index('col')
    n_rows, n_cols = 4, 4

    def load(src, b, slot):
        return pltpu.make_async_copy(src.at[pl.ds(b * STAGE_ROWS, STAGE_ROWS)], stage.at[slot], in_sems.at[slot])

    blocks = EXT_ROWS // STAGE_ROWS
    load(image, 0, 0).start()

    strip = lax.broadcasted_iota(jnp.int32, (PAD_STEPS, STRIPS, CH), 1)
    step = lax.broadcasted_iota(jnp.int32, (PAD_STEPS, STRIPS, CH), 0) - 1
    column = strip * STEPS + step
    own = (column >= COL_HALO) & (column < COL_HALO + TILE)
    own_mask[...] = own.astype(F32).astype(BF16)
    lowest = jnp.where(col_id == 0, COL_HALO, -1)
    highest = jnp.where(col_id == n_cols - 1, COL_HALO + TILE, EXT_COLS + 1)
    img_mask[...] = ((column >= lowest) & (column < highest)).astype(F32).astype(BF16)

    for i, (w_ref, back) in enumerate(((w_first, False), (w_second, False), (w_third, False), (w_third, True), (w_second, True), (w_first, True))):
        pack_weights(w_ref, wp.at[i], back)

    zero_row = jnp.zeros((PAD_STEPS, STRIPS, CH), BF16)
    xp[0, 1] = zero_row
    xp[PAIRS + 1, 0] = zero_row
    d_two[0, 1] = zero_row
    d_two[PAIRS - 1, 0] = zero_row
    wide[:, 0:8] = jnp.zeros((STAGE_ROWS, 8, CH), F32)
    wide[:, EXT_COLS + 8:EXT_COLS + 16] = jnp.zeros((STAGE_ROWS, 8, CH), F32)

    def to_strips(src, dst, off, nxt):
        def body(b, carry):
            slot = lax.rem(b, 2)

            @pl.when(b + 1 < blocks)
            def _():
                load(src, b + 1, 1 - slot).start()
            if nxt is not None:
                @pl.when(b + 1 == blocks)
                def _():
                    load(nxt, 0, 1 - slot).start()
            load(src, b, slot).wait()
            for r in range(STAGE_ROWS):
                wide[r, 8:8 + EXT_COLS] = stage[slot, r].astype(F32)
            for r in range(STAGE_ROWS):
                tiles = [wide[r, pl.ds(7 + t, STRIPS, stride=STEPS)] for t in range(PAD_STEPS)]
                dst[off + b * (STAGE_ROWS // 2) + r // 2, r % 2] = jnp.stack(tiles).astype(BF16)
            return carry
        return body

    lax.fori_loop(0, blocks, to_strips(image, xp, 1, None), 0)
    load(grad, 0, 0).start()
    lax.fori_loop(0, blocks, to_strips(grad, gp, 0, None), 0)

    def mask_rows(ref):
        zeros = jnp.zeros((2, 2, PAD_STEPS, STRIPS, CH), BF16)

        @pl.when(row_id == 0)
        def _():
            ref[0:2] = zeros

        @pl.when(row_id == n_rows - 1)
        def _():
            ref[PAIRS - 2:PAIRS] = zeros

    def forward_epilogue(pre, post):
        def epilogue(k, par, j, value):
            rounded = value.astype(BF16)
            pre[k, par] = rounded
            post[k, par] = with_edges(gelu_tanh(rounded.astype(F32))).astype(BF16) * img_mask[...]
        return epilogue

    def backward_epilogue(pre, post):
        def epilogue(k, par, j, value):
            slope = gelu_slope(pre[k, par].astype(F32))
            post[k, par] = with_edges(value * slope).astype(BF16) * img_mask[...]
        return epilogue

    conv_stage(xp, 1, wp.at[0], 0, PAIRS, 17, forward_epilogue(a_one, one))
    mask_rows(one)
    conv_stage(one, 0, wp.at[1], 1, PAIRS - 2, 11, forward_epilogue(a_two, two))
    mask_rows(two)
    conv_stage(gp, 0, wp.at[3], 1, PAIRS - 2, 11, backward_epilogue(a_two, d_two))
    mask_rows(d_two)
    wgrad_stage(two, 0, gp, own_mask, acc, dw_third, 16)
    conv_stage(d_two, 0, wp.at[4], 1, PAIRS - 2, 11, backward_epilogue(a_one, d_one))
    mask_rows(d_one)
    wgrad_stage(one, 0, d_two, own_mask, acc, dw_second, 16)
    wgrad_stage(xp, 1, d_one, own_mask, acc, dw_first, 16)

    per_out = 4
    out_steps = OWN_PAIRS // per_out

    def store(dst, s, slot):
        return pltpu.make_async_copy(outs.at[slot], dst.at[pl.ds(s * 2 * per_out, 2 * per_out)], out_sems.at[slot])

    def final_stage(src, wp_ref, skip, skip_off, dst):
        def body(s, carry):
            slot = lax.rem(s, 2)

            @pl.when(s >= 2)
            def _():
                store(dst, s - 2, slot).wait()
            base = FIRST_OWN + s * per_out
            for j in range(per_out):
                k = base + j
                parts = []
                for q in range(3):
                    for r in range(4):
                        pair, par = row_at(src, k, r, 0)
                        parts.append(src[pair, par, q:q + STEPS].reshape(STEPS * STRIPS, CH))
                res = jnp.dot(jnp.concatenate(parts, axis=1), wp_ref[...], preferred_element_type=F32)
                for par in range(2):
                    value = res[:, par * CH:(par + 1) * CH].reshape(STEPS, STRIPS, CH) + skip[k + skip_off, par, 1:1 + STEPS].astype(F32)
                    line = 2 * j + par
                    for t in range(STEPS):
                        wide[line, pl.ds(8 + t, STRIPS, stride=STEPS)] = value[t]
                    outs[slot, line] = wide[line, 8 + COL_HALO:8 + COL_HALO + TILE].astype(BF16)
            store(dst, s, slot).start()
            return carry
        lax.fori_loop(0, out_steps, body, 0)
        for s in range(out_steps - 2, out_steps):
            store(dst, s, s % 2).wait()

    final_stage(two, wp.at[2], xp, 1, block_out)
    final_stage(d_one, wp.at[5], gp, 0, grad_image)


def border_pad(tile, n_rows, n_cols):
    down_pairs = [(source, source + 1) for source in range(n_rows - 1)]
    up_pairs = [(source + 1, source) for source in range(n_rows - 1)]
    from_above = lax.ppermute(tile[tile.shape[0] - ROW_HALO:], 'row', down_pairs)
    from_below = lax.ppermute(tile[:ROW_HALO], 'row', up_pairs)
    taller = jnp.concatenate([from_above, tile, from_below], axis=0)
    right_pairs = [(source, source + 1) for source in range(n_cols - 1)]
    left_pairs = [(source + 1, source) for source in range(n_cols - 1)]
    from_left = lax.ppermute(taller[:, taller.shape[1] - COL_HALO:], 'col', right_pairs)
    from_right = lax.ppermute(taller[:, :COL_HALO], 'col', left_pairs)
    return jnp.concatenate([from_left, taller, from_right], axis=1)


def solution(mesh):
    n_rows = mesh.shape['row']
    n_cols = mesh.shape['col']
    act_spec = P(None, 'row', 'col', None)
    padded = (PAIRS, 2, PAD_STEPS, STRIPS, CH)
    plain = (PAIRS, 2, STEPS, STRIPS, CH)
    tile_shape = jax.ShapeDtypeStruct((TILE, TILE, CH), BF16)
    dw_shape = jax.ShapeDtypeStruct((3, 3, CH, CH), F32)
    hbm = pl.BlockSpec(memory_space=pl.ANY)
    vmem = pl.BlockSpec(memory_space=pltpu.VMEM)
    call = pl.pallas_call(
        block_kernel,
        out_shape=(tile_shape, tile_shape, dw_shape, dw_shape, dw_shape),
        in_specs=[hbm, hbm, vmem, vmem, vmem],
        out_specs=(hbm, hbm, vmem, vmem, vmem),
        scratch_shapes=[
            pltpu.VMEM((PAIRS + 2, 2, PAD_STEPS, STRIPS, CH), BF16),
            pltpu.VMEM(padded, BF16), pltpu.VMEM(padded, BF16), pltpu.VMEM(padded, BF16),
            pltpu.VMEM(padded, BF16), pltpu.VMEM(padded, BF16),
            pltpu.VMEM(plain, BF16), pltpu.VMEM(plain, BF16),
            pltpu.VMEM((6, 12 * CH, 2 * CH), BF16),
            pltpu.VMEM((2, STAGE_ROWS, EXT_COLS, CH), BF16),
            pltpu.VMEM((STAGE_ROWS, EXT_COLS + 16, CH), F32),
            pltpu.VMEM((2, 8, TILE, CH), BF16),
            pltpu.VMEM((3 * CH, 3 * CH), F32),
            pltpu.VMEM((PAD_STEPS, STRIPS, CH), BF16),
            pltpu.VMEM((PAD_STEPS, STRIPS, CH), BF16),
            pltpu.SemaphoreType.DMA((2,)),
            pltpu.SemaphoreType.DMA((2,)),
        ],
        compiler_params=pltpu.CompilerParams(vmem_limit_bytes=67043328),
        name='block',
    )

    def local_block(image, w_first, w_second, w_third, grad_out):
        image_ext = border_pad(image[0], n_rows, n_cols)
        grad_ext = border_pad(grad_out[0], n_rows, n_cols)
        out, dx, dw1, dw2, dw3 = call(image_ext, grad_ext, w_first, w_second, w_third)
        dw1, dw2, dw3 = lax.psum((dw1, dw2, dw3), ('row', 'col'))
        return out[None], dx[None], dw1, dw2, dw3

    return jax.shard_map(local_block, mesh=mesh, in_specs=(act_spec, P(), P(), P(), act_spec), out_specs=(act_spec, act_spec, P(), P(), P()), check_vma=False)
```

```python
import functools
import math
import jax
import jax.numpy as jnp
from jax import lax
from jax.experimental import pallas as pl
from jax.experimental.pallas import tpu as pltpu
from jax.sharding import PartitionSpec as P

GELU_SCALE = math.sqrt(2.0 / math.pi)
GELU_CUBIC = 0.044715
BF16 = jnp.bfloat16
F32 = jnp.float32

TILE = 128
CH = 128
ROW_HALO = 4
COL_HALO = 8
STRIPS = 16
STEPS = 9
PAD_STEPS = STEPS + 2
PAIRS = 68
FIRST_OWN = ROW_HALO // 2
OWN_PAIRS = TILE // 2
EXT_ROWS = TILE + 2 * ROW_HALO
EXT_COLS = TILE + 2 * COL_HALO
STAGE_ROWS = 8
QUAD = 4
N_ROWS = 4
N_COLS = 4
CHUNK = 9 * CH // (N_ROWS * N_COLS)


def gelu_tanh(value):
    return 0.5 * value * (1.0 + jnp.tanh(GELU_SCALE * (value + GELU_CUBIC * value * value * value)))


def gelu_slope(value):
    tanh_val = jnp.tanh(GELU_SCALE * (value + GELU_CUBIC * value * value * value))
    return 0.5 * (1.0 + tanh_val) + 0.5 * value * (1.0 - tanh_val * tanh_val) * GELU_SCALE * (1.0 + 3.0 * GELU_CUBIC * value * value)


def row_at(ref, k, r, off):
    pair = k - 1 if r == 0 else k + 1 if r == 3 else k
    return pair + off, (r + 1) % 2


def pack_weights(w_ref, wp_ref, back):
    zero = jnp.zeros((CH, CH), BF16)
    for q in range(3):
        for p in range(3):
            if back:
                block = w_ref[2 - p, 2 - q].astype(F32).T.astype(BF16)
            else:
                block = w_ref[p, q]
            for b in range(2):
                wp_ref[pl.ds((q * 4 + p + b) * CH, CH), pl.ds(b * CH, CH)] = block
        wp_ref[pl.ds((q * 4 + 3) * CH, CH), pl.ds(0, CH)] = zero
        wp_ref[pl.ds((q * 4) * CH, CH), pl.ds(CH, CH)] = zero


def conv_stage(src, off, wp, first, count, per_step, epilogue):
    def body(step, carry):
        base = first + step * per_step
        for j in range(per_step):
            k = base + j
            parts = []
            for q in range(3):
                for r in range(4):
                    pair, par = row_at(src, k, r, off)
                    parts.append(src[pair, par, q:q + STEPS].reshape(STEPS * STRIPS, CH))
            acc = jnp.dot(jnp.concatenate(parts, axis=1), wp[...], preferred_element_type=F32)
            for par in range(2):
                epilogue(k, par, j, acc[:, par * CH:(par + 1) * CH].reshape(STEPS, STRIPS, CH))
        return carry
    lax.fori_loop(0, count // per_step, body, 0)


def with_edges(value):
    left = pltpu.roll(value[STEPS - 1], 1, 0)[None]
    right = pltpu.roll(value[0], STRIPS - 1, 0)[None]
    return jnp.concatenate([left, value, right], axis=0)


def wgrad_stage(val, off, grad, own_mask, acc, out, per_step):
    dims = (((0,), (0,)), ((), ()))
    flat = per_step * STEPS * STRIPS
    acc[...] = jnp.zeros_like(acc)

    def rows_of(k, r):
        pair, par = row_at(val, k, r, off)
        return val[pl.ds(pair, per_step), par, 1:1 + STEPS].reshape(flat, CH)

    def body(step, carry):
        k = FIRST_OWN + step * per_step
        rows = [rows_of(k, r) for r in range(4)]
        shifted = []
        for par in range(2):
            d = grad[pl.ds(k, per_step), par] * own_mask[...][None]
            shifted.append([d[:, 2 - q:2 - q + STEPS].reshape(flat, CH) for q in range(3)])
        lhs = jnp.concatenate([jnp.concatenate(rows[par:par + 3], axis=1) for par in range(2)], axis=0)
        rhs = jnp.concatenate([jnp.concatenate(shifted[par][:2], axis=1) for par in range(2)], axis=0)
        acc[:, 0:2 * CH] += lax.dot_general(lhs, rhs, dims, preferred_element_type=F32)
        both = jnp.concatenate([shifted[0][2], shifted[1][2]], axis=1)
        last = lax.dot_general(jnp.concatenate(rows, axis=1), both, dims, preferred_element_type=F32)
        acc[:, 2 * CH:3 * CH] += last[0:3 * CH, 0:CH] + last[CH:4 * CH, CH:2 * CH]
        return carry

    lax.fori_loop(0, OWN_PAIRS // per_step, body, 0)
    for p in range(3):
        for q in range(3):
            out[(p * 3 + q) * CH:(p * 3 + q + 1) * CH] = acc[p * CH:(p + 1) * CH, q * CH:(q + 1) * CH]


def directions():
    return [(dr, dc) for dr in (-1, 0, 1) for dc in (-1, 0, 1) if (dr, dc) != (0, 0)]


def block_kernel(image, image_quads, image_pairs, grad, grad_quads, grad_pairs, w_first, w_second, w_third,
                 block_out, grad_image, dw_first, dw_second, dw_third,
                 xp, one, two, gp, d_two, d_one, a_one, a_two, wp,
                 halo, wide, outs, acc, img_mask, own_mask, part, got, final,
                 in_sems, out_sems, halo_send, halo_recv, sum_send, sum_recv, all_send, all_recv):
    n_rows, n_cols = N_ROWS, N_COLS
    n_dev = n_rows * n_cols
    row_id = lax.axis_index('row')
    col_id = lax.axis_index('col')
    me = col_id * n_rows + row_id

    def local(i):
        src, dst = ((image_pairs, d_one), (grad_pairs, d_two))[i]
        return pltpu.make_async_copy(src, dst.at[pl.ds(FIRST_OWN, OWN_PAIRS), :, pl.ds(0, 8)], in_sems.at[i])

    local(0).start()
    local(1).start()

    barrier = pltpu.get_barrier_semaphore()

    def device(d):
        other = lax.rem(me + d, n_dev)
        return other, {'col': other // n_rows, 'row': lax.rem(other, n_rows)}

    def greet(d, carry):
        pl.semaphore_signal(barrier, inc=1, device_id=device(d)[1], device_id_type=pl.DeviceIdType.MESH)
        return carry
    lax.fori_loop(1, n_dev, greet, 0)

    strip = lax.broadcasted_iota(jnp.int32, (PAD_STEPS, STRIPS, CH), 1)
    step = lax.broadcasted_iota(jnp.int32, (PAD_STEPS, STRIPS, CH), 0) - 1
    column = strip * STEPS + step
    own = (column >= COL_HALO) & (column < COL_HALO + TILE)
    own_mask[...] = own.astype(F32).astype(BF16)
    lowest = jnp.where(col_id == 0, COL_HALO, -1)
    highest = jnp.where(col_id == n_cols - 1, COL_HALO + TILE, EXT_COLS + 1)
    img_mask[...] = ((column >= lowest) & (column < highest)).astype(F32).astype(BF16)
    zero_row = jnp.zeros((PAD_STEPS, STRIPS, CH), BF16)
    xp[0, 1] = zero_row
    xp[PAIRS + 1, 0] = zero_row
    wide[:, 0:16] = jnp.zeros((STAGE_ROWS, 16, CH), F32)
    wide[:, TILE + 16:TILE + 32] = jnp.zeros((STAGE_ROWS, 16, CH), F32)

    @pl.when(col_id == 0)
    def _():
        halo[0, 0] = jnp.zeros((EXT_ROWS, QUAD, CH), BF16)
        halo[1, 0] = jnp.zeros((EXT_ROWS, QUAD, CH), BF16)

    @pl.when(col_id == n_cols - 1)
    def _():
        halo[0, 1] = jnp.zeros((EXT_ROWS, QUAD, CH), BF16)
        halo[1, 1] = jnp.zeros((EXT_ROWS, QUAD, CH), BF16)

    pl.semaphore_wait(barrier, n_dev - 1)

    def halo_copy(i, n, dr, dc):
        quads, pairs, natural = ((image_quads, image_pairs, d_one), (grad_quads, grad_pairs, d_two))[i]
        if dc == 0:
            src = pairs.at[pl.ds(0, 2)] if dr < 0 else pairs.at[pl.ds(OWN_PAIRS - 2, 2)]
            dst = natural.at[pl.ds(PAIRS - 2, 2) if dr < 0 else pl.ds(0, 2), :, pl.ds(0, 8)]
        else:
            rows = (pl.ds(0, ROW_HALO), pl.ds(0, TILE), pl.ds(TILE - ROW_HALO, ROW_HALO))[dr + 1]
            into = (pl.ds(EXT_ROWS - ROW_HALO, ROW_HALO), pl.ds(ROW_HALO, TILE), pl.ds(0, ROW_HALO))[dr + 1]
            src = quads.at[rows, 0 if dc < 0 else TILE // QUAD - 1]
            dst = halo.at[i, 1 if dc < 0 else 0, into]
        return pltpu.make_async_remote_copy(
            src_ref=src, dst_ref=dst, send_sem=halo_send.at[i, n], recv_sem=halo_recv.at[i, n],
            device_id={'col': col_id + dc, 'row': row_id + dr}, device_id_type=pl.DeviceIdType.MESH)

    def exists(dr, dc):
        ok = None
        for pos, shift, size in ((row_id, dr, n_rows), (col_id, dc, n_cols)):
            if shift:
                one_ok = (pos + shift >= 0) & (pos + shift < size)
                ok = one_ok if ok is None else ok & one_ok
        return ok

    for i in range(2):
        for n, (dr, dc) in enumerate(directions()):
            @pl.when(exists(dr, dc))
            def _():
                halo_copy(i, n, dr, dc).start()

    for i, (w_ref, back) in enumerate(((w_first, False), (w_second, False), (w_third, False), (w_third, True), (w_second, True), (w_first, True))):
        pack_weights(w_ref, wp.at[i], back)

    def halo_wait(i):
        for n, (dr, dc) in enumerate(directions()):
            @pl.when(exists(-dr, -dc))
            def _():
                halo_copy(i, n, dr, dc).wait_recv()

    def mask_rows(ref, off=0):
        zeros = jnp.zeros((2, 2, PAD_STEPS, STRIPS, CH), BF16)

        @pl.when(row_id == 0)
        def _():
            ref[off:off + 2] = zeros

        @pl.when(row_id == n_rows - 1)
        def _():
            ref[off + PAIRS - 2:off + PAIRS] = zeros

    def to_strips(i, natural, dst, off):
        local(i).wait()
        halo_wait(i)

        def body(b, carry):
            for r in range(STAGE_ROWS):
                k, par = b * (STAGE_ROWS // 2) + r // 2, r % 2
                wide[r, 16:16 + TILE] = natural[k, par, 0:8].reshape(TILE, CH).astype(F32)
                wide[r, 16 - QUAD:16] = halo[i, 0, 2 * k + par].astype(F32)
                wide[r, 16 + TILE:16 + TILE + QUAD] = halo[i, 1, 2 * k + par].astype(F32)
            for r in range(STAGE_ROWS):
                k, par = b * (STAGE_ROWS // 2) + r // 2, r % 2
                tiles = [wide[r, pl.ds(7 + t, STRIPS, stride=STEPS)] for t in range(PAD_STEPS)]
                dst[off + k, par] = jnp.stack(tiles).astype(BF16)
            return carry
        lax.fori_loop(0, EXT_ROWS // STAGE_ROWS, body, 0)
        mask_rows(dst, off)

    def forward_epilogue(pre, post):
        def epilogue(k, par, j, value):
            rounded = value.astype(BF16)
            pre[k, par] = rounded
            post[k, par] = with_edges(gelu_tanh(rounded.astype(F32))).astype(BF16) * img_mask[...]
        return epilogue

    def backward_epilogue(pre, post):
        def epilogue(k, par, j, value):
            slope = gelu_slope(pre[k, par].astype(F32))
            post[k, par] = with_edges(value * slope).astype(BF16) * img_mask[...]
        return epilogue

    def sum_start(i):
        def body(d, carry):
            other, ids = device(d)
            pltpu.make_async_remote_copy(
                src_ref=part.at[i, pl.ds(other * CHUNK, CHUNK)], dst_ref=got.at[i, d - 1],
                send_sem=sum_send.at[i], recv_sem=sum_recv.at[i],
                device_id=ids, device_id_type=pl.DeviceIdType.MESH).start()
            return carry
        lax.fori_loop(1, n_dev, body, 0)

    def wait_all(i, sem):
        pltpu.make_async_copy(got.at[i], got.at[i], sem.at[i]).wait()

    def sum_finish(i):
        wait_all(i, sum_recv)
        mine = pl.ds(me * CHUNK, CHUNK)
        total = part[i, mine]
        for d in range(n_dev - 1):
            total = total + got[i, d]
        final[i, mine] = total

    def spread_start(i):
        mine = pl.ds(me * CHUNK, CHUNK)

        def body(d, carry):
            pltpu.make_async_remote_copy(
                src_ref=final.at[i, mine], dst_ref=final.at[i, mine],
                send_sem=all_send.at[i], recv_sem=all_recv.at[i],
                device_id=device(d)[1], device_id_type=pl.DeviceIdType.MESH).start()
            return carry
        lax.fori_loop(1, n_dev, body, 0)

    grads_out = (dw_first, dw_second, dw_third)

    def spread_finish(i):
        wait_all(i, all_recv)
        return pltpu.make_async_copy(final.at[i], grads_out[i], in_sems.at[2 + i])

    to_strips(0, d_one, xp, 1)
    conv_stage(xp, 1, wp.at[0], 0, PAIRS, 17, forward_epilogue(a_one, one))
    mask_rows(one)
    conv_stage(one, 0, wp.at[1], 1, PAIRS - 2, 11, forward_epilogue(a_two, two))
    mask_rows(two)
    to_strips(1, d_two, gp, 0)
    d_two[0, 1] = zero_row
    d_two[PAIRS - 1, 0] = zero_row
    conv_stage(gp, 0, wp.at[3], 1, PAIRS - 2, 11, backward_epilogue(a_two, d_two))
    mask_rows(d_two)
    wgrad_stage(two, 0, gp, own_mask, acc, part.at[2], 16)
    conv_stage(d_two, 0, wp.at[4], 1, 22, 11, backward_epilogue(a_one, d_one))
    sum_start(2)
    conv_stage(d_two, 0, wp.at[4], 23, 44, 11, backward_epilogue(a_one, d_one))
    mask_rows(d_one)
    wgrad_stage(one, 0, d_two, own_mask, acc, part.at[1], 16)
    sum_finish(2)
    wgrad_stage(xp, 1, d_one, own_mask, acc, part.at[0], 16)
    spread_start(2)
    sum_start(1)

    per_out = 4
    out_steps = OWN_PAIRS // per_out

    def store(dst, s, slot):
        return pltpu.make_async_copy(outs.at[slot], dst.at[pl.ds(s * 2 * per_out, 2 * per_out)], out_sems.at[slot])

    def final_stage(src, wp_ref, skip, skip_off, dst, hooks):
        def body(s, carry):
            slot = lax.rem(s, 2)

            @pl.when(s >= 2)
            def _():
                store(dst, s - 2, slot).wait()
            base = FIRST_OWN + s * per_out
            for j in range(per_out):
                k = base + j
                parts = []
                for q in range(3):
                    for r in range(4):
                        pair, par = row_at(src, k, r, 0)
                        parts.append(src[pair, par, q:q + STEPS].reshape(STEPS * STRIPS, CH))
                res = jnp.dot(jnp.concatenate(parts, axis=1), wp_ref[...], preferred_element_type=F32)
                for par in range(2):
                    value = res[:, par * CH:(par + 1) * CH].reshape(STEPS, STRIPS, CH) + skip[k + skip_off, par, 1:1 + STEPS].astype(F32)
                    line = 2 * j + par
                    for t in range(STEPS):
                        wide[line, pl.ds(8 + t, STRIPS, stride=STEPS)] = value[t]
                    outs[slot, line] = wide[line, 8 + COL_HALO:8 + COL_HALO + TILE].astype(BF16)
            store(dst, s, slot).start()
            return carry
        start = 0
        for stop, hook in list(hooks) + [(out_steps, None)]:
            lax.fori_loop(start, stop, body, 0)
            if hook is not None:
                hook()
            start = stop
        for s in range(out_steps - 2, out_steps):
            store(dst, s, s % 2).wait()

    def mid_one():
        sum_start(0)

    def mid_two():
        sum_finish(1)

    final_stage(two, wp.at[2], xp, 1, block_out, [(1, mid_one), (15, mid_two)])
    spread_start(1)
    sum_finish(0)
    copy_three = spread_finish(2)
    copy_three.start()
    final_stage(d_one, wp.at[5], gp, 0, grad_image, [(1, lambda: spread_start(0))])
    copy_two = spread_finish(1)
    copy_two.start()
    copy_one = spread_finish(0)
    copy_one.start()
    for i in range(3):
        wait_all(i, sum_send)
        wait_all(i, all_send)
    for i in range(2):
        for n, (dr, dc) in enumerate(directions()):
            @pl.when(exists(dr, dc))
            def _():
                halo_copy(i, n, dr, dc).wait_send()
    copy_three.wait()
    copy_two.wait()
    copy_one.wait()


def solution(mesh):
    assert (mesh.shape['row'], mesh.shape['col']) == (N_ROWS, N_COLS)
    act_spec = P(None, 'row', 'col', None)
    padded = (PAIRS, 2, PAD_STEPS, STRIPS, CH)
    plain = (PAIRS, 2, STEPS, STRIPS, CH)
    tile_shape = jax.ShapeDtypeStruct((TILE, TILE, CH), BF16)
    dw_shape = jax.ShapeDtypeStruct((9 * CH, CH), F32)
    hbm = pl.BlockSpec(memory_space=pl.ANY)
    vmem = pl.BlockSpec(memory_space=pltpu.VMEM)
    n_dev = N_ROWS * N_COLS
    call = pl.pallas_call(
        block_kernel,
        out_shape=(tile_shape, tile_shape, dw_shape, dw_shape, dw_shape),
        in_specs=[hbm] * 6 + [vmem] * 3,
        out_specs=(hbm,) * 5,
        scratch_shapes=[
            pltpu.VMEM((PAIRS + 2, 2, PAD_STEPS, STRIPS, CH), BF16),
            pltpu.VMEM(padded, BF16), pltpu.VMEM(padded, BF16), pltpu.VMEM(padded, BF16),
            pltpu.VMEM(padded, BF16), pltpu.VMEM(padded, BF16),
            pltpu.VMEM(plain, BF16), pltpu.VMEM(plain, BF16),
            pltpu.VMEM((6, 12 * CH, 2 * CH), BF16),
            pltpu.VMEM((2, 2, EXT_ROWS, QUAD, CH), BF16),
            pltpu.VMEM((STAGE_ROWS, EXT_COLS + 16, CH), F32),
            pltpu.VMEM((2, 8, TILE, CH), BF16),
            pltpu.VMEM((3 * CH, 3 * CH), F32),
            pltpu.VMEM((PAD_STEPS, STRIPS, CH), BF16),
            pltpu.VMEM((PAD_STEPS, STRIPS, CH), BF16),
            pltpu.VMEM((3, 9 * CH, CH), F32),
            pltpu.VMEM((3, n_dev - 1, CHUNK, CH), F32),
            pltpu.VMEM((3, 9 * CH, CH), F32),
            pltpu.SemaphoreType.DMA((5,)),
            pltpu.SemaphoreType.DMA((2,)),
            pltpu.SemaphoreType.DMA((2, 8)),
            pltpu.SemaphoreType.DMA((2, 8)),
            pltpu.SemaphoreType.DMA((3,)),
            pltpu.SemaphoreType.DMA((3,)),
            pltpu.SemaphoreType.DMA((3,)),
            pltpu.SemaphoreType.DMA((3,)),
        ],
        compiler_params=pltpu.CompilerParams(vmem_limit_bytes=67043328, collective_id=0, has_side_effects=True),
        name='block',
    )

    def local_block(image, w_first, w_second, w_third, grad_out):
        views = []
        for tile in (image, grad_out):
            views += [tile.reshape(TILE, TILE, CH), tile.reshape(TILE, TILE // QUAD, QUAD, CH), tile.reshape(OWN_PAIRS, 2, TILE // STRIPS, STRIPS, CH)]
        out, dx, dw1, dw2, dw3 = call(*views, w_first, w_second, w_third)
        shape = (3, 3, CH, CH)
        return out[None], dx[None], dw1.reshape(shape), dw2.reshape(shape), dw3.reshape(shape)

    return jax.shard_map(local_block, mesh=mesh, in_specs=(act_spec, P(), P(), P(), act_spec), out_specs=(act_spec, act_spec, P(), P(), P()), check_vma=False)
```

```python
import functools
import math
import jax
import jax.numpy as jnp
from jax import lax
from jax.experimental import pallas as pl
from jax.experimental.pallas import tpu as pltpu
from jax.sharding import PartitionSpec as P

GELU_SCALE = math.sqrt(2.0 / math.pi)
GELU_CUBIC = 0.044715
BF16 = jnp.bfloat16
F32 = jnp.float32

TILE = 128
CH = 128
ROW_HALO = 4
COL_HALO = 8
STRIPS = 16
STEPS = 9
PAD_STEPS = STEPS + 2
PAIRS = 68
FIRST_OWN = ROW_HALO // 2
OWN_PAIRS = TILE // 2
EXT_ROWS = TILE + 2 * ROW_HALO
EXT_COLS = TILE + 2 * COL_HALO
QUAD = 4
N_ROWS = 4
N_COLS = 4
SIDES = 4
SIDE_ROWS = TILE // SIDES
HALF = 9 * CH // 2
CHUNK = 9 * CH // (N_ROWS * N_COLS)


def gelu_tanh(value):
    return 0.5 * value * (1.0 + jnp.tanh(GELU_SCALE * (value + GELU_CUBIC * value * value * value)))


def gelu_slope(value):
    tanh_val = jnp.tanh(GELU_SCALE * (value + GELU_CUBIC * value * value * value))
    return 0.5 * (1.0 + tanh_val) + 0.5 * value * (1.0 - tanh_val * tanh_val) * GELU_SCALE * (1.0 + 3.0 * GELU_CUBIC * value * value)


def row_at(ref, k, r, off):
    pair = k - 1 if r == 0 else k + 1 if r == 3 else k
    return pair + off, (r + 1) % 2


def pack_weights(w_ref, wp_ref, back):
    zero = jnp.zeros((CH, CH), BF16)
    for q in range(3):
        for p in range(3):
            if back:
                block = w_ref[2 - p, 2 - q].astype(F32).T.astype(BF16)
            else:
                block = w_ref[p, q]
            for b in range(2):
                wp_ref[pl.ds((q * 4 + p + b) * CH, CH), pl.ds(b * CH, CH)] = block
        wp_ref[pl.ds((q * 4 + 3) * CH, CH), pl.ds(0, CH)] = zero
        wp_ref[pl.ds((q * 4) * CH, CH), pl.ds(CH, CH)] = zero


def run_hooks(hooks, step):
    for at, hook in hooks:
        @pl.when(step == at)
        def _():
            hook()


def conv_stage(src, off, wp, first, count, per_step, epilogue, hooks=()):
    def body(step, carry):
        base = first + step * per_step
        for j in range(per_step):
            k = base + j
            parts = []
            for q in range(3):
                for r in range(4):
                    pair, par = row_at(src, k, r, off)
                    parts.append(src[pair, par, q:q + STEPS].reshape(STEPS * STRIPS, CH))
            acc = jnp.dot(jnp.concatenate(parts, axis=1), wp[...], preferred_element_type=F32)
            for par in range(2):
                epilogue(k, par, j, acc[:, par * CH:(par + 1) * CH].reshape(STEPS, STRIPS, CH))
        run_hooks(hooks, step)
        return carry
    lax.fori_loop(0, count // per_step, body, 0)


def with_edges(value):
    left = pltpu.roll(value[STEPS - 1], 1, 0)[None]
    right = pltpu.roll(value[0], STRIPS - 1, 0)[None]
    return jnp.concatenate([left, value, right], axis=0)


def wgrad_stage(val, off, grad, own_mask, acc, out, per_step, hooks=()):
    dims = (((0,), (0,)), ((), ()))
    flat = per_step * STEPS * STRIPS
    acc[...] = jnp.zeros_like(acc)

    def rows_of(k, r):
        pair, par = row_at(val, k, r, off)
        return val[pl.ds(pair, per_step), par, 1:1 + STEPS].reshape(flat, CH)

    def body(step, carry):
        k = FIRST_OWN + step * per_step
        rows = [rows_of(k, r) for r in range(4)]
        shifted = []
        for par in range(2):
            d = grad[pl.ds(k, per_step), par] * own_mask[...][None]
            shifted.append([d[:, 2 - q:2 - q + STEPS].reshape(flat, CH) for q in range(3)])
        lhs = jnp.concatenate([jnp.concatenate(rows[par:par + 3], axis=1) for par in range(2)], axis=0)
        rhs = jnp.concatenate([jnp.concatenate(shifted[par][:2], axis=1) for par in range(2)], axis=0)
        acc[:, 0:2 * CH] += lax.dot_general(lhs, rhs, dims, preferred_element_type=F32)
        both = jnp.concatenate([shifted[0][2], shifted[1][2]], axis=1)
        last = lax.dot_general(jnp.concatenate(rows, axis=1), both, dims, preferred_element_type=F32)
        acc[:, 2 * CH:3 * CH] += last[0:3 * CH, 0:CH] + last[CH:4 * CH, CH:2 * CH]
        run_hooks(hooks, step)
        return carry

    lax.fori_loop(0, OWN_PAIRS // per_step, body, 0)
    for p in range(3):
        for q in range(3):
            out[(p * 3 + q) * CH:(p * 3 + q + 1) * CH] = acc[p * CH:(p + 1) * CH, q * CH:(q + 1) * CH]


def directions():
    return [(dr, dc) for dr in (-1, 0, 1) for dc in (-1, 0, 1) if (dr, dc) != (0, 0)]


def block_kernel(image, image_quads, image_pairs, grad, grad_quads, grad_pairs, w_first, w_second, w_third,
                 block_out, grad_image, dw_first, dw_second, dw_third,
                 xp, one, two, gp, d_two, d_one, a_one, a_two, wp,
                 halo, wide, outs, acc, img_mask, own_mask, part, pair_got, half, got, final,
                 in_sems, out_sems, halo_send, halo_recv, sum_send, sum_recv):
    n_rows, n_cols = N_ROWS, N_COLS
    n_dev = n_rows * n_cols
    row_id = lax.axis_index('row')
    col_id = lax.axis_index('col')
    me = col_id * n_rows + row_id

    def local(i):
        src, dst = ((image_pairs, d_one), (grad_pairs, d_two))[i]
        return pltpu.make_async_copy(src, dst.at[pl.ds(FIRST_OWN, OWN_PAIRS), :, pl.ds(0, 8)], in_sems.at[i])

    local(0).start()
    local(1).start()

    barrier = pltpu.get_barrier_semaphore()

    def device(d):
        other = lax.rem(me + d, n_dev)
        return other, {'col': other // n_rows, 'row': lax.rem(other, n_rows)}

    def greet(d, carry):
        pl.semaphore_signal(barrier, inc=1, device_id=device(d)[1], device_id_type=pl.DeviceIdType.MESH)
        return carry
    lax.fori_loop(1, n_dev, greet, 0)

    strip = lax.broadcasted_iota(jnp.int32, (PAD_STEPS, STRIPS, CH), 1)
    step = lax.broadcasted_iota(jnp.int32, (PAD_STEPS, STRIPS, CH), 0) - 1
    column = strip * STEPS + step
    own = (column >= COL_HALO) & (column < COL_HALO + TILE)
    own_mask[...] = own.astype(F32).astype(BF16)
    lowest = jnp.where(col_id == 0, COL_HALO, -1)
    highest = jnp.where(col_id == n_cols - 1, COL_HALO + TILE, EXT_COLS + 1)
    img_mask[...] = ((column >= lowest) & (column < highest)).astype(F32).astype(BF16)
    zero_row = jnp.zeros((PAD_STEPS, STRIPS, CH), BF16)
    xp[0, 1] = zero_row
    xp[PAIRS + 1, 0] = zero_row
    wide[:, 0:16] = jnp.zeros((16, 16, CH), F32)
    wide[:, TILE + 16:TILE + 32] = jnp.zeros((16, 16, CH), F32)

    @pl.when(col_id == 0)
    def _():
        halo[0, 0] = jnp.zeros((EXT_ROWS, QUAD, CH), BF16)
        halo[1, 0] = jnp.zeros((EXT_ROWS, QUAD, CH), BF16)

    @pl.when(col_id == n_cols - 1)
    def _():
        halo[0, 1] = jnp.zeros((EXT_ROWS, QUAD, CH), BF16)
        halo[1, 1] = jnp.zeros((EXT_ROWS, QUAD, CH), BF16)

    pl.semaphore_wait(barrier, n_dev - 1)

    def halo_copy(i, n, dr, dc, chunk=0):
        quads, pairs, natural = ((image_quads, image_pairs, d_one), (grad_quads, grad_pairs, d_two))[i]
        if dc == 0:
            src = pairs.at[pl.ds(0, 2)] if dr < 0 else pairs.at[pl.ds(OWN_PAIRS - 2, 2)]
            dst = natural.at[pl.ds(PAIRS - 2, 2) if dr < 0 else pl.ds(0, 2), :, pl.ds(0, 8)]
        else:
            side = pl.ds(chunk * SIDE_ROWS, SIDE_ROWS)
            rows = (pl.ds(0, ROW_HALO), side, pl.ds(TILE - ROW_HALO, ROW_HALO))[dr + 1]
            into = (pl.ds(EXT_ROWS - ROW_HALO, ROW_HALO), pl.ds(ROW_HALO + chunk * SIDE_ROWS, SIDE_ROWS), pl.ds(0, ROW_HALO))[dr + 1]
            src = quads.at[rows, 0 if dc < 0 else TILE // QUAD - 1]
            dst = halo.at[i, 1 if dc < 0 else 0, into]
        return pltpu.make_async_remote_copy(
            src_ref=src, dst_ref=dst, send_sem=halo_send.at[i, n, chunk], recv_sem=halo_recv.at[i, n, chunk],
            device_id={'col': col_id + dc, 'row': row_id + dr}, device_id_type=pl.DeviceIdType.MESH)

    def exists(dr, dc):
        ok = None
        for pos, shift, size in ((row_id, dr, n_rows), (col_id, dc, n_cols)):
            if shift:
                one_ok = (pos + shift >= 0) & (pos + shift < size)
                ok = one_ok if ok is None else ok & one_ok
        return ok

    around = list(enumerate(directions()))
    sides = [(n, d) for n, d in around if d[0] == 0]
    over = [(n, d) for n, d in around if d[0] == 1]
    under = [(n, d) for n, d in around if d[0] == -1]

    def halo_do(i, group, chunk, what):
        for n, (dr, dc) in group:
            flip = -1 if what == 'recv' else 1

            @pl.when(exists(flip * dr, flip * dc))
            def _():
                copy = halo_copy(i, n, dr, dc, chunk)
                if what == 'start':
                    copy.start()
                elif what == 'recv':
                    copy.wait_recv()
                else:
                    copy.wait_send()

    def halo_start(i):
        halo_do(i, over, 0, 'start')
        for chunk in range(SIDES):
            halo_do(i, sides, chunk, 'start')
        halo_do(i, under, 0, 'start')

    halo_start(0)

    for i, (w_ref, back) in enumerate(((w_first, False), (w_second, False), (w_third, False), (w_third, True), (w_second, True), (w_first, True))):
        pack_weights(w_ref, wp.at[i], back)

    def mask_rows(ref, off=0):
        zeros = jnp.zeros((2, 2, PAD_STEPS, STRIPS, CH), BF16)

        @pl.when(row_id == 0)
        def _():
            ref[off:off + 2] = zeros

        @pl.when(row_id == n_rows - 1)
        def _():
            ref[off + PAIRS - 2:off + PAIRS] = zeros

    def to_strips(i, natural, dst, off, first, count):
        def body(b, carry):
            for r in range(4):
                k, par = first + 2 * b + r // 2, r % 2
                wide[r, 16:16 + TILE] = natural[k, par, 0:8].reshape(TILE, CH).astype(F32)
                wide[r, 16 - QUAD:16] = halo[i, 0, 2 * k + par].astype(F32)
                wide[r, 16 + TILE:16 + TILE + QUAD] = halo[i, 1, 2 * k + par].astype(F32)
            for r in range(4):
                k, par = first + 2 * b + r // 2, r % 2
                tiles = [wide[r, pl.ds(7 + t, STRIPS, stride=STEPS)] for t in range(PAD_STEPS)]
                dst[off + k, par] = jnp.stack(tiles).astype(BF16)
            return carry
        lax.fori_loop(0, count // 2, body, 0)

    def forward_epilogue(pre, post):
        def epilogue(k, par, j, value):
            rounded = value.astype(BF16)
            pre[k, par] = rounded
            post[k, par] = with_edges(gelu_tanh(rounded.astype(F32))).astype(BF16) * img_mask[...]
        return epilogue

    def backward_epilogue(pre, post):
        def epilogue(k, par, j, value):
            slope = gelu_slope(pre[k, par].astype(F32))
            post[k, par] = with_edges(value * slope).astype(BF16) * img_mask[...]
        return epilogue

    core = lax.rem(row_id, 2)
    chip = col_id * 2 + row_id // 2
    n_chips = n_dev // 2
    partner = {'col': col_id, 'row': row_id + 1 - 2 * core}
    my_half = pl.ds(core * HALF, HALF)
    mine = pl.ds(core * HALF + chip * CHUNK, CHUNK)
    MESH = pl.DeviceIdType.MESH
    grads_out = (dw_first, dw_second, dw_third)

    def pair_copy(i):
        return pltpu.make_async_remote_copy(
            src_ref=part.at[i, pl.ds((1 - core) * HALF, HALF)], dst_ref=pair_got.at[i],
            send_sem=sum_send.at[i, 0], recv_sem=sum_recv.at[i, 0], device_id=partner, device_id_type=MESH)

    def pair_start(i):
        pair_copy(i).start()

    def pair_add(i):
        pair_copy(i).wait_recv()
        half[i] = part[i, my_half] + pair_got[i]

    def to_chips(make):
        def body(d, carry):
            other = lax.rem(chip + d, n_chips)
            make(d, other, {'col': other // 2, 'row': lax.rem(other, 2) * 2 + core}).start()
            return carry
        lax.fori_loop(1, n_chips, body, 0)

    def chunk_start(i):
        to_chips(lambda d, other, ids: pltpu.make_async_remote_copy(
            src_ref=half.at[i, pl.ds(other * CHUNK, CHUNK)], dst_ref=got.at[i, d - 1],
            send_sem=sum_send.at[i, 1], recv_sem=sum_recv.at[i, 1], device_id=ids, device_id_type=MESH))

    def wait_bytes(i, sem):
        pltpu.make_async_copy(got.at[i], got.at[i], sem).wait()

    def chunk_add(i):
        wait_bytes(i, sum_recv.at[i, 1])
        total = half[i, pl.ds(chip * CHUNK, CHUNK)]
        for d in range(n_chips - 1):
            total = total + got[i, d]
        final[i, mine] = total

    def spread_start(i):
        to_chips(lambda d, other, ids: pltpu.make_async_remote_copy(
            src_ref=final.at[i, mine], dst_ref=final.at[i, mine],
            send_sem=sum_send.at[i, 2], recv_sem=sum_recv.at[i, 2], device_id=ids, device_id_type=MESH))

    def return_copy(i):
        return pltpu.make_async_remote_copy(
            src_ref=final.at[i, my_half], dst_ref=final.at[i, my_half],
            send_sem=sum_send.at[i, 3], recv_sem=sum_recv.at[i, 3], device_id=partner, device_id_type=MESH)

    def return_start(i):
        wait_bytes(i, sum_recv.at[i, 2])
        return_copy(i).start()

    def out_copy(i):
        return pltpu.make_async_copy(final.at[i], grads_out[i], in_sems.at[2 + i])

    def out_start(i):
        return_copy(i).wait_recv()
        out_copy(i).start()

    local(0).wait()
    halo_do(0, over, 0, 'recv')
    to_strips(0, d_one, xp, 1, 0, 2)
    first_step = forward_epilogue(a_one, one)

    def first_body(c, carry):
        halo_do(0, sides, c, 'recv')
        to_strips(0, d_one, xp, 1, 2 + c * 16, 16)

        @pl.when((c == 0) & (row_id == 0))
        def _():
            xp[1:3] = jnp.zeros((2, 2, PAD_STEPS, STRIPS, CH), BF16)
        conv_stage(xp, 1, wp.at[0], c * 16, 16, 16, first_step)
        return carry
    lax.fori_loop(0, SIDES, first_body, 0)
    halo_do(0, under, 0, 'recv')
    halo_start(1)
    to_strips(0, d_one, xp, 1, PAIRS - 2, 2)
    mask_rows(xp, 1)
    conv_stage(xp, 1, wp.at[0], 64, 4, 4, first_step)
    mask_rows(one)
    conv_stage(one, 0, wp.at[1], 1, PAIRS - 2, 11, forward_epilogue(a_two, two))
    mask_rows(two)
    local(1).wait()
    halo_do(1, over, 0, 'recv')
    for chunk in range(SIDES):
        halo_do(1, sides, chunk, 'recv')
    halo_do(1, under, 0, 'recv')
    to_strips(1, d_two, gp, 0, 0, PAIRS)
    mask_rows(gp)
    d_two[0, 1] = zero_row
    d_two[PAIRS - 1, 0] = zero_row
    conv_stage(gp, 0, wp.at[3], 1, PAIRS - 2, 11, backward_epilogue(a_two, d_two))
    mask_rows(d_two)

    def call(fn, i):
        return lambda: fn(i)

    wgrad_stage(two, 0, gp, own_mask, acc, part.at[2], 16)
    conv_stage(d_two, 0, wp.at[4], 1, PAIRS - 2, 11, backward_epilogue(a_one, d_one),
               [(0, call(pair_start, 2)), (2, call(pair_add, 2)), (3, call(chunk_start, 2))])
    mask_rows(d_one)
    wgrad_stage(one, 0, d_two, own_mask, acc, part.at[1], 16, [(2, call(chunk_add, 2)), (3, call(spread_start, 2))])
    wgrad_stage(xp, 1, d_one, own_mask, acc, part.at[0], 16,
                [(0, call(pair_start, 1)), (1, call(pair_add, 1)), (2, call(chunk_start, 1)), (3, call(return_start, 2))])

    per_out = 8
    out_steps = OWN_PAIRS // per_out

    def store(dst, s, slot):
        return pltpu.make_async_copy(outs.at[slot], dst.at[pl.ds(s * 2 * per_out, 2 * per_out)], out_sems.at[slot])

    def final_stage(src, wp_ref, skip, skip_off, dst, hooks):
        def body(s, carry):
            slot = lax.rem(s, 2)

            @pl.when(s >= 2)
            def _():
                store(dst, s - 2, slot).wait()
            base = FIRST_OWN + s * per_out
            for j in range(per_out):
                k = base + j
                parts = []
                for q in range(3):
                    for r in range(4):
                        pair, par = row_at(src, k, r, 0)
                        parts.append(src[pair, par, q:q + STEPS].reshape(STEPS * STRIPS, CH))
                res = jnp.dot(jnp.concatenate(parts, axis=1), wp_ref[...], preferred_element_type=F32)
                for par in range(2):
                    value = res[:, par * CH:(par + 1) * CH].reshape(STEPS, STRIPS, CH) + skip[k + skip_off, par, 1:1 + STEPS].astype(F32)
                    line = 2 * j + par
                    for t in range(STEPS):
                        wide[line, pl.ds(8 + t, STRIPS, stride=STEPS)] = value[t]
                    outs[slot, line] = wide[line, 8 + COL_HALO:8 + COL_HALO + TILE].astype(BF16)
            store(dst, s, slot).start()
            run_hooks(hooks, s)
            return carry
        lax.fori_loop(0, out_steps, body, 0)
        for s in range(out_steps - 2, out_steps):
            store(dst, s, s % 2).wait()

    final_stage(two, wp.at[2], xp, 1, block_out,
                [(0, call(pair_start, 0)), (1, call(pair_add, 0)), (2, call(chunk_start, 0)), (3, call(chunk_add, 1)),
                 (4, call(spread_start, 1)), (5, call(out_start, 2)), (7, call(chunk_add, 0))])
    final_stage(d_one, wp.at[5], gp, 0, grad_image,
                [(0, call(spread_start, 0)), (3, call(return_start, 1)), (5, call(out_start, 1)), (6, call(return_start, 0))])
    out_start(0)
    for i in range(3):
        pair_copy(i).wait_send()
        wait_bytes(i, sum_send.at[i, 1])
        wait_bytes(i, sum_send.at[i, 2])
        return_copy(i).wait_send()
    for i in range(2):
        halo_do(i, over, 0, 'send')
        for chunk in range(SIDES):
            halo_do(i, sides, chunk, 'send')
        halo_do(i, under, 0, 'send')
    for i in range(3):
        out_copy(i).wait()


def solution(mesh):
    assert (mesh.shape['row'], mesh.shape['col']) == (N_ROWS, N_COLS)
    act_spec = P(None, 'row', 'col', None)
    padded = (PAIRS, 2, PAD_STEPS, STRIPS, CH)
    plain = (PAIRS, 2, STEPS, STRIPS, CH)
    tile_shape = jax.ShapeDtypeStruct((TILE, TILE, CH), BF16)
    dw_shape = jax.ShapeDtypeStruct((9 * CH, CH), F32)
    hbm = pl.BlockSpec(memory_space=pl.ANY)
    vmem = pl.BlockSpec(memory_space=pltpu.VMEM)
    n_dev = N_ROWS * N_COLS
    call = pl.pallas_call(
        block_kernel,
        out_shape=(tile_shape, tile_shape, dw_shape, dw_shape, dw_shape),
        in_specs=[hbm] * 6 + [vmem] * 3,
        out_specs=(hbm,) * 5,
        scratch_shapes=[
            pltpu.VMEM((PAIRS + 2, 2, PAD_STEPS, STRIPS, CH), BF16),
            pltpu.VMEM(padded, BF16), pltpu.VMEM(padded, BF16), pltpu.VMEM(padded, BF16),
            pltpu.VMEM(padded, BF16), pltpu.VMEM(padded, BF16),
            pltpu.VMEM(plain, BF16), pltpu.VMEM(plain, BF16),
            pltpu.VMEM((6, 12 * CH, 2 * CH), BF16),
            pltpu.VMEM((2, 2, EXT_ROWS, QUAD, CH), BF16),
            pltpu.VMEM((16, EXT_COLS + 16, CH), F32),
            pltpu.VMEM((2, 16, TILE, CH), BF16),
            pltpu.VMEM((3 * CH, 3 * CH), F32),
            pltpu.VMEM((PAD_STEPS, STRIPS, CH), BF16),
            pltpu.VMEM((PAD_STEPS, STRIPS, CH), BF16),
            pltpu.VMEM((3, 9 * CH, CH), F32),
            pltpu.VMEM((3, HALF, CH), F32),
            pltpu.VMEM((3, HALF, CH), F32),
            pltpu.VMEM((3, n_dev // 2 - 1, CHUNK, CH), F32),
            pltpu.VMEM((3, 9 * CH, CH), F32),
            pltpu.SemaphoreType.DMA((5,)),
            pltpu.SemaphoreType.DMA((2,)),
            pltpu.SemaphoreType.DMA((2, 8, SIDES)),
            pltpu.SemaphoreType.DMA((2, 8, SIDES)),
            pltpu.SemaphoreType.DMA((3, 4)),
            pltpu.SemaphoreType.DMA((3, 4)),
        ],
        compiler_params=pltpu.CompilerParams(vmem_limit_bytes=67043328, collective_id=0, has_side_effects=True),
        name='block',
    )

    def local_block(image, w_first, w_second, w_third, grad_out):
        views = []
        for tile in (image, grad_out):
            views += [tile.reshape(TILE, TILE, CH), tile.reshape(TILE, TILE // QUAD, QUAD, CH), tile.reshape(OWN_PAIRS, 2, TILE // STRIPS, STRIPS, CH)]
        out, dx, dw1, dw2, dw3 = call(*views, w_first, w_second, w_third)
        shape = (3, 3, CH, CH)
        return out[None], dx[None], dw1.reshape(shape), dw2.reshape(shape), dw3.reshape(shape)

    return jax.shard_map(local_block, mesh=mesh, in_specs=(act_spec, P(), P(), P(), act_spec), out_specs=(act_spec, act_spec, P(), P(), P()), check_vma=False)
```

```python
import functools
import math
import jax
import jax.numpy as jnp
from jax import lax
from jax.experimental import pallas as pl
from jax.experimental.pallas import tpu as pltpu
from jax.sharding import PartitionSpec as P

GELU_SCALE = math.sqrt(2.0 / math.pi)
GELU_CUBIC = 0.044715
BF16 = jnp.bfloat16
F32 = jnp.float32

TILE = 128
CH = 128
ROW_HALO = 4
COL_HALO = 8
STRIPS = 16
STEPS = 9
PAD_STEPS = STEPS + 2
PAIRS = 68
FIRST_OWN = ROW_HALO // 2
OWN_PAIRS = TILE // 2
EXT_ROWS = TILE + 2 * ROW_HALO
EXT_COLS = TILE + 2 * COL_HALO
QUAD = 4
N_ROWS = 4
N_COLS = 4
PIECES = 4
COPY_PARTS = (8, 8, 1, 1, 1)
SIDES = 4
SIDE_ROWS = TILE // SIDES
HALF = 9 * CH // 2
CHUNK = 9 * CH // (N_ROWS * N_COLS)


def gelu_arg(value, square):
    return jnp.tanh(value * (GELU_SCALE + (GELU_SCALE * GELU_CUBIC) * square))


def gelu_tanh(value):
    return 0.5 * value * (1.0 + gelu_arg(value, value * value))


def gelu_slope(value):
    square = value * value
    s = 0.5 + 0.5 * gelu_arg(value, square)
    return s + (s * (1.0 - s) * value) * (2.0 * GELU_SCALE + (6.0 * GELU_SCALE * GELU_CUBIC) * square)


def row_at(ref, k, r, off):
    pair = k - 1 if r == 0 else k + 1 if r == 3 else k
    return pair + off, (r + 1) % 2


def pack_weights(w_ref, wp_ref, back):
    zero = jnp.zeros((CH, CH), BF16)
    for q in range(3):
        for p in range(3):
            if back:
                block = w_ref[2 - p, 2 - q].astype(F32).T.astype(BF16)
            else:
                block = w_ref[p, q]
            for b in range(2):
                wp_ref[pl.ds((q * 4 + p + b) * CH, CH), pl.ds(b * CH, CH)] = block
        wp_ref[pl.ds((q * 4 + 3) * CH, CH), pl.ds(0, CH)] = zero
        wp_ref[pl.ds((q * 4) * CH, CH), pl.ds(CH, CH)] = zero


def run_hooks(hooks, step):
    for at, hook in hooks:
        @pl.when(step == at)
        def _():
            hook()


def conv_stage(src, off, wp, first, count, per_step, epilogue, hooks=()):
    def body(step, carry):
        base = first + step * per_step
        for j in range(per_step):
            k = base + j
            parts = []
            for q in range(3):
                for r in range(4):
                    pair, par = row_at(src, k, r, off)
                    parts.append(src[pair, par, q:q + STEPS].reshape(STEPS * STRIPS, CH))
            acc = jnp.dot(jnp.concatenate(parts, axis=1), wp[...], preferred_element_type=F32)
            for par in range(2):
                epilogue(k, par, j, acc[:, par * CH:(par + 1) * CH].reshape(STEPS, STRIPS, CH))
        run_hooks(hooks, step)
        return carry
    lax.fori_loop(0, count // per_step, body, 0)


def with_edges(value):
    left = pltpu.roll(value[STEPS - 1], 1, 0)[None]
    right = pltpu.roll(value[0], STRIPS - 1, 0)[None]
    return jnp.concatenate([left, value, right], axis=0)


def wgrad_stage(val, off, grad, own_mask, acc, out, per_step, hooks=()):
    dims = (((0,), (0,)), ((), ()))
    flat = per_step * STEPS * STRIPS
    acc[...] = jnp.zeros_like(acc)

    def rows_of(k, r):
        pair, par = row_at(val, k, r, off)
        return val[pl.ds(pair, per_step), par, 1:1 + STEPS].reshape(flat, CH)

    def body(step, carry):
        k = FIRST_OWN + step * per_step
        rows = [rows_of(k, r) for r in range(4)]
        shifted = []
        for par in range(2):
            d = grad[pl.ds(k, per_step), par] * own_mask[...][None]
            shifted.append([d[:, 2 - q:2 - q + STEPS].reshape(flat, CH) for q in range(3)])
        lhs = jnp.concatenate([jnp.concatenate(rows[par:par + 3], axis=1) for par in range(2)], axis=0)
        rhs = jnp.concatenate([jnp.concatenate(shifted[par][:2], axis=1) for par in range(2)], axis=0)
        acc[:, 0:2 * CH] += lax.dot_general(lhs, rhs, dims, preferred_element_type=F32)
        both = jnp.concatenate([shifted[0][2], shifted[1][2]], axis=1)
        last = lax.dot_general(jnp.concatenate(rows, axis=1), both, dims, preferred_element_type=F32)
        acc[:, 2 * CH:3 * CH] += last[0:3 * CH, 0:CH] + last[CH:4 * CH, CH:2 * CH]
        run_hooks(hooks, step)
        return carry

    lax.fori_loop(0, OWN_PAIRS // per_step, body, 0)
    for p in range(3):
        for q in range(3):
            out[(p * 3 + q) * CH:(p * 3 + q + 1) * CH] = acc[p * CH:(p + 1) * CH, q * CH:(q + 1) * CH]


def directions():
    return [(dr, dc) for dr in (-1, 0, 1) for dc in (-1, 0, 1) if (dr, dc) != (0, 0)]


def block_kernel(image, image_quads, image_pairs, grad, grad_quads, grad_pairs, w_first, w_second, w_third,
                 block_out, grad_image, dw_first, dw_second, dw_third,
                 xp, one, two, gp, d_two, d_one, a_one, a_two, wp,
                 halo, wide, outs, acc, img_mask, own_mask, part, pair_got, half, got, final,
                 in_sems, out_sems, halo_send, halo_recv, sum_send, sum_recv):
    n_rows, n_cols = N_ROWS, N_COLS
    n_dev = n_rows * n_cols
    row_id = lax.axis_index('row')
    col_id = lax.axis_index('col')
    me = col_id * n_rows + row_id

    def local(i):
        src, dst = ((image_pairs, d_one), (grad_pairs, d_two))[i]
        return pltpu.make_async_copy(src, dst.at[pl.ds(FIRST_OWN, OWN_PAIRS), :, pl.ds(0, 8)], in_sems.at[i])

    local(0).start()
    local(1).start()

    barrier = pltpu.get_barrier_semaphore()

    def device(d):
        other = lax.rem(me + d, n_dev)
        return other, {'col': other // n_rows, 'row': lax.rem(other, n_rows)}

    def greet(d, carry):
        pl.semaphore_signal(barrier, inc=1, device_id=device(d)[1], device_id_type=pl.DeviceIdType.MESH)
        return carry
    lax.fori_loop(1, n_dev, greet, 0)

    strip = lax.broadcasted_iota(jnp.int32, (PAD_STEPS, STRIPS, CH), 1)
    step = lax.broadcasted_iota(jnp.int32, (PAD_STEPS, STRIPS, CH), 0) - 1
    column = strip * STEPS + step
    own = (column >= COL_HALO) & (column < COL_HALO + TILE)
    own_mask[...] = own.astype(F32).astype(BF16)
    lowest = jnp.where(col_id == 0, COL_HALO, -1)
    highest = jnp.where(col_id == n_cols - 1, COL_HALO + TILE, EXT_COLS + 1)
    img_mask[...] = ((column >= lowest) & (column < highest)).astype(F32).astype(BF16)
    zero_row = jnp.zeros((PAD_STEPS, STRIPS, CH), BF16)
    xp[0, 1] = zero_row
    xp[PAIRS + 1, 0] = zero_row
    wide[:, 0:16] = jnp.zeros((16, 16, CH), F32)
    wide[:, TILE + 16:TILE + 32] = jnp.zeros((16, 16, CH), F32)

    @pl.when(col_id == 0)
    def _():
        halo[0, 0] = jnp.zeros((EXT_ROWS, QUAD, CH), BF16)
        halo[1, 0] = jnp.zeros((EXT_ROWS, QUAD, CH), BF16)

    @pl.when(col_id == n_cols - 1)
    def _():
        halo[0, 1] = jnp.zeros((EXT_ROWS, QUAD, CH), BF16)
        halo[1, 1] = jnp.zeros((EXT_ROWS, QUAD, CH), BF16)

    pl.semaphore_wait(barrier, n_dev - 1)

    def halo_copy(i, n, dr, dc, chunk=0):
        quads, pairs, natural = ((image_quads, image_pairs, d_one), (grad_quads, grad_pairs, d_two))[i]
        if dc == 0:
            src = pairs.at[pl.ds(0, 2)] if dr < 0 else pairs.at[pl.ds(OWN_PAIRS - 2, 2)]
            dst = natural.at[pl.ds(PAIRS - 2, 2) if dr < 0 else pl.ds(0, 2), :, pl.ds(0, 8)]
        else:
            side = pl.ds(chunk * SIDE_ROWS, SIDE_ROWS)
            rows = (pl.ds(0, ROW_HALO), side, pl.ds(TILE - ROW_HALO, ROW_HALO))[dr + 1]
            into = (pl.ds(EXT_ROWS - ROW_HALO, ROW_HALO), pl.ds(ROW_HALO + chunk * SIDE_ROWS, SIDE_ROWS), pl.ds(0, ROW_HALO))[dr + 1]
            src = quads.at[rows, 0 if dc < 0 else TILE // QUAD - 1]
            dst = halo.at[i, 1 if dc < 0 else 0, into]
        return pltpu.make_async_remote_copy(
            src_ref=src, dst_ref=dst, send_sem=halo_send.at[i, n, chunk], recv_sem=halo_recv.at[i, n, chunk],
            device_id={'col': col_id + dc, 'row': row_id + dr}, device_id_type=pl.DeviceIdType.MESH)

    def exists(dr, dc):
        ok = None
        for pos, shift, size in ((row_id, dr, n_rows), (col_id, dc, n_cols)):
            if shift:
                one_ok = (pos + shift >= 0) & (pos + shift < size)
                ok = one_ok if ok is None else ok & one_ok
        return ok

    around = list(enumerate(directions()))
    sides = [(n, d) for n, d in around if d[0] == 0]
    over = [(n, d) for n, d in around if d[0] == 1]
    under = [(n, d) for n, d in around if d[0] == -1]

    def halo_do(i, group, chunk, what):
        for n, (dr, dc) in group:
            flip = -1 if what == 'recv' else 1

            @pl.when(exists(flip * dr, flip * dc))
            def _():
                copy = halo_copy(i, n, dr, dc, chunk)
                if what == 'start':
                    copy.start()
                elif what == 'recv':
                    copy.wait_recv()
                else:
                    copy.wait_send()

    def halo_start(i):
        halo_do(i, over, 0, 'start')
        for chunk in range(SIDES):
            halo_do(i, sides, chunk, 'start')
        halo_do(i, under, 0, 'start')

    halo_start(0)

    for i, (w_ref, back) in enumerate(((w_first, False), (w_second, False), (w_third, False), (w_third, True), (w_second, True), (w_first, True))):
        pack_weights(w_ref, wp.at[i], back)

    def mask_rows(ref, off=0):
        zeros = jnp.zeros((2, 2, PAD_STEPS, STRIPS, CH), BF16)

        @pl.when(row_id == 0)
        def _():
            ref[off:off + 2] = zeros

        @pl.when(row_id == n_rows - 1)
        def _():
            ref[off + PAIRS - 2:off + PAIRS] = zeros

    def to_strips(i, natural, dst, off, first, count):
        def body(b, carry):
            for r in range(4):
                k, par = first + 2 * b + r // 2, r % 2
                wide[r, 16:16 + TILE] = natural[k, par, 0:8].reshape(TILE, CH).astype(F32)
                wide[r, 16 - QUAD:16] = halo[i, 0, 2 * k + par].astype(F32)
                wide[r, 16 + TILE:16 + TILE + QUAD] = halo[i, 1, 2 * k + par].astype(F32)
            for r in range(4):
                k, par = first + 2 * b + r // 2, r % 2
                tiles = [wide[r, pl.ds(7 + t, STRIPS, stride=STEPS)] for t in range(PAD_STEPS)]
                dst[off + k, par] = jnp.stack(tiles).astype(BF16)
            return carry
        lax.fori_loop(0, count // 2, body, 0)

    def forward_epilogue(pre, post):
        def epilogue(k, par, j, value):
            rounded = value.astype(BF16)
            pre[k, par] = rounded
            post[k, par] = with_edges(gelu_tanh(rounded.astype(F32))).astype(BF16) * img_mask[...]
        return epilogue

    def backward_epilogue(pre, post):
        def epilogue(k, par, j, value):
            slope = gelu_slope(pre[k, par].astype(F32))
            post[k, par] = with_edges(value * slope).astype(BF16) * img_mask[...]
        return epilogue

    core = lax.rem(row_id, 2)
    chip = col_id * 2 + row_id // 2
    n_chips = n_dev // 2
    partner = {'col': col_id, 'row': row_id + 1 - 2 * core}
    my_half = pl.ds(core * HALF, HALF)
    mine = pl.ds(core * HALF + chip * CHUNK, CHUNK)
    MESH = pl.DeviceIdType.MESH
    grads_out = (dw_first, dw_second, dw_third)

    def pieces(make):
        for n in range(PIECES):
            make(n * (HALF // PIECES), HALF // PIECES).start()

    def wait_half(i, sem):
        pltpu.make_async_copy(half.at[i], half.at[i], sem).wait()

    def pair_start(i):
        pieces(lambda at, size: pltpu.make_async_remote_copy(
            src_ref=part.at[i, pl.ds((1 - core) * HALF + at, size)], dst_ref=pair_got.at[i, pl.ds(at, size)],
            send_sem=sum_send.at[i, 0], recv_sem=sum_recv.at[i, 0], device_id=partner, device_id_type=MESH))

    def pair_add(i):
        wait_half(i, sum_recv.at[i, 0])
        half[i] = part[i, my_half] + pair_got[i]

    def to_chips(make):
        def body(d, carry):
            other = lax.rem(chip + d, n_chips)
            make(d, other, {'col': other // 2, 'row': lax.rem(other, 2) * 2 + core}).start()
            return carry
        lax.fori_loop(1, n_chips, body, 0)

    def chunk_start(i):
        to_chips(lambda d, other, ids: pltpu.make_async_remote_copy(
            src_ref=half.at[i, pl.ds(other * CHUNK, CHUNK)], dst_ref=got.at[i, d - 1],
            send_sem=sum_send.at[i, 1], recv_sem=sum_recv.at[i, 1], device_id=ids, device_id_type=MESH))

    def wait_bytes(i, sem):
        pltpu.make_async_copy(got.at[i], got.at[i], sem).wait()

    def chunk_add(i):
        wait_bytes(i, sum_recv.at[i, 1])
        total = half[i, pl.ds(chip * CHUNK, CHUNK)]
        for d in range(n_chips - 1):
            total = total + got[i, d]
        final[i, mine] = total

    def spread_start(i):
        to_chips(lambda d, other, ids: pltpu.make_async_remote_copy(
            src_ref=final.at[i, mine], dst_ref=final.at[i, mine],
            send_sem=sum_send.at[i, 2], recv_sem=sum_recv.at[i, 2], device_id=ids, device_id_type=MESH))

    def return_start(i):
        wait_bytes(i, sum_recv.at[i, 2])
        pieces(lambda at, size: pltpu.make_async_remote_copy(
            src_ref=final.at[i, pl.ds(core * HALF + at, size)], dst_ref=final.at[i, pl.ds(core * HALF + at, size)],
            send_sem=sum_send.at[i, 3], recv_sem=sum_recv.at[i, 3], device_id=partner, device_id_type=MESH))

    def out_copy(i):
        return pltpu.make_async_copy(final.at[i], grads_out[i], in_sems.at[2 + i])

    def out_start(i):
        wait_half(i, sum_recv.at[i, 3])
        out_copy(i).start()

    local(0).wait()
    halo_do(0, over, 0, 'recv')
    to_strips(0, d_one, xp, 1, 0, 2)
    first_step = forward_epilogue(a_one, one)

    def first_body(c, carry):
        halo_do(0, sides, c, 'recv')
        to_strips(0, d_one, xp, 1, 2 + c * 16, 16)

        @pl.when((c == 0) & (row_id == 0))
        def _():
            xp[1:3] = jnp.zeros((2, 2, PAD_STEPS, STRIPS, CH), BF16)
        conv_stage(xp, 1, wp.at[0], c * 16, 16, 16, first_step)
        return carry
    lax.fori_loop(0, SIDES, first_body, 0)
    halo_do(0, under, 0, 'recv')
    halo_start(1)
    to_strips(0, d_one, xp, 1, PAIRS - 2, 2)
    mask_rows(xp, 1)
    conv_stage(xp, 1, wp.at[0], 64, 4, 4, first_step)
    mask_rows(one)
    conv_stage(one, 0, wp.at[1], 1, PAIRS - 2, 22, forward_epilogue(a_two, two))
    mask_rows(two)
    local(1).wait()
    halo_do(1, over, 0, 'recv')
    for chunk in range(SIDES):
        halo_do(1, sides, chunk, 'recv')
    halo_do(1, under, 0, 'recv')
    to_strips(1, d_two, gp, 0, 0, PAIRS)
    mask_rows(gp)
    d_two[0, 1] = zero_row
    d_two[PAIRS - 1, 0] = zero_row
    conv_stage(gp, 0, wp.at[3], 1, PAIRS - 2, 22, backward_epilogue(a_two, d_two))
    mask_rows(d_two)

    def call(fn, i):
        return lambda: fn(i)

    wgrad_stage(two, 0, gp, own_mask, acc, part.at[2], 16)
    pair_start(2)
    wgrad_stage(one, 0, d_two, own_mask, acc, part.at[1], 16,
                [(1, call(pair_add, 2)), (1, call(chunk_start, 2))])
    pair_start(1)
    conv_stage(d_two, 0, wp.at[4], 1, PAIRS - 2, 22, backward_epilogue(a_one, d_one),
               [(0, call(pair_add, 1)), (0, call(chunk_start, 1)), (1, call(chunk_add, 2)), (1, call(spread_start, 2))])
    mask_rows(d_one)
    wgrad_stage(xp, 1, d_one, own_mask, acc, part.at[0], 16,
                [(1, call(chunk_add, 1)), (1, call(spread_start, 1)), (3, call(return_start, 2))])
    pair_start(0)

    per_out = 8
    out_steps = OWN_PAIRS // per_out

    def store(dst, s, slot):
        return pltpu.make_async_copy(outs.at[slot], dst.at[pl.ds(s * 2 * per_out, 2 * per_out)], out_sems.at[slot])

    def final_stage(src, wp_ref, skip, skip_off, dst, hooks):
        def body(s, carry):
            slot = lax.rem(s, 2)

            @pl.when(s >= 2)
            def _():
                store(dst, s - 2, slot).wait()
            base = FIRST_OWN + s * per_out
            for j in range(per_out):
                k = base + j
                parts = []
                for q in range(3):
                    for r in range(4):
                        pair, par = row_at(src, k, r, 0)
                        parts.append(src[pair, par, q:q + STEPS].reshape(STEPS * STRIPS, CH))
                res = jnp.dot(jnp.concatenate(parts, axis=1), wp_ref[...], preferred_element_type=F32)
                for par in range(2):
                    value = res[:, par * CH:(par + 1) * CH].reshape(STEPS, STRIPS, CH) + skip[k + skip_off, par, 1:1 + STEPS].astype(F32)
                    line = 2 * j + par
                    for t in range(STEPS):
                        wide[line, pl.ds(8 + t, STRIPS, stride=STEPS)] = value[t]
                    outs[slot, line] = wide[line, 8 + COL_HALO:8 + COL_HALO + TILE].astype(BF16)
            store(dst, s, slot).start()
            run_hooks(hooks, s)
            return carry
        lax.fori_loop(0, out_steps, body, 0)
        for s in range(out_steps - 2, out_steps):
            store(dst, s, s % 2).wait()

    final_stage(two, wp.at[2], xp, 1, block_out,
                [(1, call(pair_add, 0)), (1, call(chunk_start, 0)), (4, call(out_start, 2)), (6, call(return_start, 1)),
                 (7, call(chunk_add, 0)), (7, call(spread_start, 0))])
    final_stage(d_one, wp.at[5], gp, 0, grad_image,
                [(1, call(out_start, 1)), (5, call(return_start, 0))])
    out_start(0)
    for i in range(3):
        wait_half(i, sum_send.at[i, 0])
        wait_bytes(i, sum_send.at[i, 1])
        wait_bytes(i, sum_send.at[i, 2])
        wait_half(i, sum_send.at[i, 3])
    for i in range(2):
        halo_do(i, over, 0, 'send')
        for chunk in range(SIDES):
            halo_do(i, sides, chunk, 'send')
        halo_do(i, under, 0, 'send')
    for i in range(3):
        out_copy(i).wait()


def copy_kernel(*refs):
    count = len(COPY_PARTS)
    srcs, dsts, bufs = refs[:count], refs[count:2 * count], refs[2 * count:3 * count]
    in_sems, out_sems = refs[3 * count:]
    moves = []
    for a, parts in enumerate(COPY_PARTS):
        rows = srcs[a].shape[0] // parts
        for b in range(parts):
            piece = pl.ds(b * rows, rows)
            n = len(moves)
            moves.append((pltpu.make_async_copy(srcs[a].at[piece], bufs[a].at[piece], in_sems.at[n]),
                          pltpu.make_async_copy(bufs[a].at[piece], dsts[a].at[piece], out_sems.at[n])))
    for into, _ in moves:
        into.start()
    for into, back in moves:
        into.wait()
        back.start()
    for _, back in moves:
        back.wait()


def solution(mesh):
    assert (mesh.shape['row'], mesh.shape['col']) == (N_ROWS, N_COLS)
    act_spec = P(None, 'row', 'col', None)
    padded = (PAIRS, 2, PAD_STEPS, STRIPS, CH)
    plain = (PAIRS, 2, STEPS, STRIPS, CH)
    tile_shape = jax.ShapeDtypeStruct((TILE, TILE, CH), BF16)
    dw_shape = jax.ShapeDtypeStruct((9 * CH, CH), F32)
    hbm = pl.BlockSpec(memory_space=pl.ANY)
    vmem = pl.BlockSpec(memory_space=pltpu.VMEM)
    n_dev = N_ROWS * N_COLS
    call = pl.pallas_call(
        block_kernel,
        out_shape=(tile_shape, tile_shape, dw_shape, dw_shape, dw_shape),
        in_specs=[hbm] * 6 + [vmem] * 3,
        out_specs=(hbm,) * 5,
        scratch_shapes=[
            pltpu.VMEM((PAIRS + 2, 2, PAD_STEPS, STRIPS, CH), BF16),
            pltpu.VMEM(padded, BF16), pltpu.VMEM(padded, BF16), pltpu.VMEM(padded, BF16),
            pltpu.VMEM(padded, BF16), pltpu.VMEM(padded, BF16),
            pltpu.VMEM(plain, BF16), pltpu.VMEM(plain, BF16),
            pltpu.VMEM((6, 12 * CH, 2 * CH), BF16),
            pltpu.VMEM((2, 2, EXT_ROWS, QUAD, CH), BF16),
            pltpu.VMEM((16, EXT_COLS + 16, CH), F32),
            pltpu.VMEM((2, 16, TILE, CH), BF16),
            pltpu.VMEM((3 * CH, 3 * CH), F32),
            pltpu.VMEM((PAD_STEPS, STRIPS, CH), BF16),
            pltpu.VMEM((PAD_STEPS, STRIPS, CH), BF16),
            pltpu.VMEM((3, 9 * CH, CH), F32),
            pltpu.VMEM((3, HALF, CH), F32),
            pltpu.VMEM((3, HALF, CH), F32),
            pltpu.VMEM((3, n_dev // 2 - 1, CHUNK, CH), F32),
            pltpu.VMEM((3, 9 * CH, CH), F32),
            pltpu.SemaphoreType.DMA((5,)),
            pltpu.SemaphoreType.DMA((2,)),
            pltpu.SemaphoreType.DMA((2, 8, SIDES)),
            pltpu.SemaphoreType.DMA((2, 8, SIDES)),
            pltpu.SemaphoreType.DMA((3, 4)),
            pltpu.SemaphoreType.DMA((3, 4)),
        ],
        compiler_params=pltpu.CompilerParams(vmem_limit_bytes=67043328, collective_id=0, has_side_effects=True),
        name='block',
    )

    copy = pl.pallas_call(
        copy_kernel,
        out_shape=(tile_shape, tile_shape, dw_shape, dw_shape, dw_shape),
        in_specs=[hbm] * 5,
        out_specs=(hbm,) * 5,
        scratch_shapes=[pltpu.VMEM(tile_shape.shape, BF16)] * 2 + [pltpu.VMEM(dw_shape.shape, F32)] * 3
        + [pltpu.SemaphoreType.DMA((sum(COPY_PARTS),))] * 2,
        compiler_params=pltpu.CompilerParams(vmem_limit_bytes=67043328),
        name='hand_over',
    )

    def local_block(image, w_first, w_second, w_third, grad_out):
        views = []
        for tile in (image, grad_out):
            views += [tile.reshape(TILE, TILE, CH), tile.reshape(TILE, TILE // QUAD, QUAD, CH), tile.reshape(OWN_PAIRS, 2, TILE // STRIPS, STRIPS, CH)]
        out, dx, dw1, dw2, dw3 = copy(*call(*views, w_first, w_second, w_third))
        shape = (3, 3, CH, CH)
        return out[None], dx[None], dw1.reshape(shape), dw2.reshape(shape), dw3.reshape(shape)

    return jax.shard_map(local_block, mesh=mesh, in_specs=(act_spec, P(), P(), P(), act_spec), out_specs=(act_spec, act_spec, P(), P(), P()), check_vma=False)
```

```python
import functools
import math
import jax
import jax.numpy as jnp
from jax import lax
from jax.experimental import pallas as pl
from jax.experimental.pallas import tpu as pltpu
from jax.sharding import PartitionSpec as P

GELU_SCALE = math.sqrt(2.0 / math.pi)
GELU_CUBIC = 0.044715
BF16 = jnp.bfloat16
F32 = jnp.float32

TILE = 128
CH = 128
ROW_HALO = 4
COL_HALO = 8
STRIPS = 16
STEPS = 9
PAD_STEPS = STEPS + 2
PAIRS = 68
FIRST_OWN = ROW_HALO // 2
OWN_PAIRS = TILE // 2
EXT_ROWS = TILE + 2 * ROW_HALO
EXT_COLS = TILE + 2 * COL_HALO
QUAD = 4
N_ROWS = 4
N_COLS = 4
UNITS = ((0, 0, 6 * CH), (1, 0, 9 * CH), (2, 0, 9 * CH), (0, 6 * CH, 3 * CH))
OUT_ROWS = 16
SIDES = 4
SIDE_ROWS = TILE // SIDES
HALF = 9 * CH // 2
CHUNK = 9 * CH // (N_ROWS * N_COLS)


def gelu_arg(value, square):
    return jnp.tanh(value * (GELU_SCALE + (GELU_SCALE * GELU_CUBIC) * square))


def gelu_tanh(value):
    return 0.5 * value * (1.0 + gelu_arg(value, value * value))


def gelu_slope(value):
    square = value * value
    s = 0.5 + 0.5 * gelu_arg(value, square)
    return s + (s * (1.0 - s) * value) * (2.0 * GELU_SCALE + (6.0 * GELU_SCALE * GELU_CUBIC) * square)


def row_at(ref, k, r, off):
    pair = k - 1 if r == 0 else k + 1 if r == 3 else k
    return pair + off, (r + 1) % 2


def pack_weights(w_ref, wp_ref, back):
    zero = jnp.zeros((CH, CH), BF16)
    for q in range(3):
        for p in range(3):
            if back:
                block = w_ref[2 - p, 2 - q].astype(F32).T.astype(BF16)
            else:
                block = w_ref[p, q]
            for b in range(2):
                wp_ref[pl.ds((q * 4 + p + b) * CH, CH), pl.ds(b * CH, CH)] = block
        wp_ref[pl.ds((q * 4 + 3) * CH, CH), pl.ds(0, CH)] = zero
        wp_ref[pl.ds((q * 4) * CH, CH), pl.ds(CH, CH)] = zero


def run_hooks(hooks, step):
    for at, hook in hooks:
        @pl.when(step == at)
        def _():
            hook()


def conv_stage(src, off, wp, first, count, per_step, epilogue, hooks=()):
    def body(step, carry):
        base = first + step * per_step
        for j in range(per_step):
            k = base + j
            parts = []
            for q in range(3):
                for r in range(4):
                    pair, par = row_at(src, k, r, off)
                    parts.append(src[pair, par, q:q + STEPS].reshape(STEPS * STRIPS, CH))
            acc = jnp.dot(jnp.concatenate(parts, axis=1), wp[...], preferred_element_type=F32)
            for par in range(2):
                epilogue(k, par, j, acc[:, par * CH:(par + 1) * CH].reshape(STEPS, STRIPS, CH))
        run_hooks(hooks, step)
        return carry
    lax.fori_loop(0, count // per_step, body, 0)


def with_edges(value):
    left = pltpu.roll(value[STEPS - 1], 1, 0)[None]
    right = pltpu.roll(value[0], STRIPS - 1, 0)[None]
    return jnp.concatenate([left, value, right], axis=0)


def wgrad_stage(val, off, grad, own_mask, acc, out, per_step, hooks=(), do_pair=True, do_last=True):
    dims = (((0,), (0,)), ((), ()))
    flat = per_step * STEPS * STRIPS
    acc[...] = jnp.zeros_like(acc)

    def rows_of(k, r):
        pair, par = row_at(val, k, r, off)
        return val[pl.ds(pair, per_step), par, 1:1 + STEPS].reshape(flat, CH)

    def body(step, carry):
        k = FIRST_OWN + step * per_step
        rows = [rows_of(k, r) for r in range(4)]
        shifted = []
        for par in range(2):
            d = grad[pl.ds(k, per_step), par] * own_mask[...][None]
            shifted.append([d[:, 2 - q:2 - q + STEPS].reshape(flat, CH) for q in range(3)])
        if do_pair:
            lhs = jnp.concatenate([jnp.concatenate(rows[par:par + 3], axis=1) for par in range(2)], axis=0)
            rhs = jnp.concatenate([jnp.concatenate(shifted[par][:2], axis=1) for par in range(2)], axis=0)
            acc[:, 0:2 * CH] += lax.dot_general(lhs, rhs, dims, preferred_element_type=F32)
        if do_last:
            both = jnp.concatenate([shifted[0][2], shifted[1][2]], axis=1)
            last = lax.dot_general(jnp.concatenate(rows, axis=1), both, dims, preferred_element_type=F32)
            acc[:, 2 * CH:3 * CH] += last[0:3 * CH, 0:CH] + last[CH:4 * CH, CH:2 * CH]
        run_hooks(hooks, step)
        return carry

    lax.fori_loop(0, OWN_PAIRS // per_step, body, 0)
    for q in ([0, 1] if do_pair else []) + ([2] if do_last else []):
        out[q * 3 * CH:(q + 1) * 3 * CH] = acc[:, q * CH:(q + 1) * CH]


def directions():
    return [(dr, dc) for dr in (-1, 0, 1) for dc in (-1, 0, 1) if (dr, dc) != (0, 0)]


def block_kernel(image, image_quads, image_pairs, grad, grad_quads, grad_pairs, w_first, w_second, w_third,
                 a_one, a_two, final,
                 xp, one, two, gp, d_two, d_one, wp,
                 halo, wide, acc, img_mask, own_mask, part, pair_got, half, got,
                 in_sems, halo_send, halo_recv, sum_send, sum_recv):
    n_rows, n_cols = N_ROWS, N_COLS
    n_dev = n_rows * n_cols
    row_id = lax.axis_index('row')
    col_id = lax.axis_index('col')
    me = col_id * n_rows + row_id

    def local(i):
        src, dst = ((image_pairs, d_one), (grad_pairs, d_two))[i]
        return pltpu.make_async_copy(src, dst.at[pl.ds(FIRST_OWN, OWN_PAIRS), :, pl.ds(0, 8)], in_sems.at[i])

    local(0).start()
    local(1).start()

    barrier = pltpu.get_barrier_semaphore()

    def device(d):
        other = lax.rem(me + d, n_dev)
        return other, {'col': other // n_rows, 'row': lax.rem(other, n_rows)}

    def greet(d, carry):
        pl.semaphore_signal(barrier, inc=1, device_id=device(d)[1], device_id_type=pl.DeviceIdType.MESH)
        return carry
    lax.fori_loop(1, n_dev, greet, 0)

    strip = lax.broadcasted_iota(jnp.int32, (PAD_STEPS, STRIPS, CH), 1)
    step = lax.broadcasted_iota(jnp.int32, (PAD_STEPS, STRIPS, CH), 0) - 1
    column = strip * STEPS + step
    own = (column >= COL_HALO) & (column < COL_HALO + TILE)
    own_mask[...] = own.astype(F32).astype(BF16)
    lowest = jnp.where(col_id == 0, COL_HALO, -1)
    highest = jnp.where(col_id == n_cols - 1, COL_HALO + TILE, EXT_COLS + 1)
    img_mask[...] = ((column >= lowest) & (column < highest)).astype(F32).astype(BF16)
    zero_row = jnp.zeros((PAD_STEPS, STRIPS, CH), BF16)
    xp[0, 1] = zero_row
    xp[PAIRS + 1, 0] = zero_row
    wide[:, 0:16] = jnp.zeros((16, 16, CH), F32)
    wide[:, TILE + 16:TILE + 32] = jnp.zeros((16, 16, CH), F32)

    @pl.when(col_id == 0)
    def _():
        halo[0, 0] = jnp.zeros((EXT_ROWS, QUAD, CH), BF16)
        halo[1, 0] = jnp.zeros((EXT_ROWS, QUAD, CH), BF16)

    @pl.when(col_id == n_cols - 1)
    def _():
        halo[0, 1] = jnp.zeros((EXT_ROWS, QUAD, CH), BF16)
        halo[1, 1] = jnp.zeros((EXT_ROWS, QUAD, CH), BF16)

    pl.semaphore_wait(barrier, n_dev - 1)

    def halo_copy(i, n, dr, dc, chunk=0):
        quads, pairs, natural = ((image_quads, image_pairs, d_one), (grad_quads, grad_pairs, d_two))[i]
        if dc == 0:
            src = pairs.at[pl.ds(0, 2)] if dr < 0 else pairs.at[pl.ds(OWN_PAIRS - 2, 2)]
            dst = natural.at[pl.ds(PAIRS - 2, 2) if dr < 0 else pl.ds(0, 2), :, pl.ds(0, 8)]
        else:
            side = pl.ds(chunk * SIDE_ROWS, SIDE_ROWS)
            rows = (pl.ds(0, ROW_HALO), side, pl.ds(TILE - ROW_HALO, ROW_HALO))[dr + 1]
            into = (pl.ds(EXT_ROWS - ROW_HALO, ROW_HALO), pl.ds(ROW_HALO + chunk * SIDE_ROWS, SIDE_ROWS), pl.ds(0, ROW_HALO))[dr + 1]
            src = quads.at[rows, 0 if dc < 0 else TILE // QUAD - 1]
            dst = halo.at[i, 1 if dc < 0 else 0, into]
        return pltpu.make_async_remote_copy(
            src_ref=src, dst_ref=dst, send_sem=halo_send.at[i, n, chunk], recv_sem=halo_recv.at[i, n, chunk],
            device_id={'col': col_id + dc, 'row': row_id + dr}, device_id_type=pl.DeviceIdType.MESH)

    def exists(dr, dc):
        ok = None
        for pos, shift, size in ((row_id, dr, n_rows), (col_id, dc, n_cols)):
            if shift:
                one_ok = (pos + shift >= 0) & (pos + shift < size)
                ok = one_ok if ok is None else ok & one_ok
        return ok

    around = list(enumerate(directions()))
    sides = [(n, d) for n, d in around if d[0] == 0]
    over = [(n, d) for n, d in around if d[0] == 1]
    under = [(n, d) for n, d in around if d[0] == -1]

    def halo_do(i, group, chunk, what):
        for n, (dr, dc) in group:
            flip = -1 if what == 'recv' else 1

            @pl.when(exists(flip * dr, flip * dc))
            def _():
                copy = halo_copy(i, n, dr, dc, chunk)
                if what == 'start':
                    copy.start()
                elif what == 'recv':
                    copy.wait_recv()
                else:
                    copy.wait_send()

    def halo_start(i):
        halo_do(i, sides, 0, 'start')
        halo_do(i, over, 0, 'start')
        for chunk in range(1, SIDES):
            halo_do(i, sides, chunk, 'start')
        halo_do(i, under, 0, 'start')

    halo_start(0)

    for i, (w_ref, back) in enumerate(((w_first, False), (w_second, False), (w_third, False), (w_third, True), (w_second, True), (w_first, True))):
        pack_weights(w_ref, wp.at[i], back)

    def mask_rows(ref, off=0):
        zeros = jnp.zeros((2, 2, PAD_STEPS, STRIPS, CH), BF16)

        @pl.when(row_id == 0)
        def _():
            ref[off:off + 2] = zeros

        @pl.when(row_id == n_rows - 1)
        def _():
            ref[off + PAIRS - 2:off + PAIRS] = zeros

    def to_strips(i, natural, dst, off, first, count):
        def body(b, carry):
            for r in range(4):
                k, par = first + 2 * b + r // 2, r % 2
                wide[r, 16:16 + TILE] = natural[k, par, 0:8].reshape(TILE, CH).astype(F32)
                wide[r, 16 - QUAD:16] = halo[i, 0, 2 * k + par].astype(F32)
                wide[r, 16 + TILE:16 + TILE + QUAD] = halo[i, 1, 2 * k + par].astype(F32)
            for r in range(4):
                k, par = first + 2 * b + r // 2, r % 2
                tiles = [wide[r, pl.ds(7 + t, STRIPS, stride=STEPS)] for t in range(PAD_STEPS)]
                dst[off + k, par] = jnp.stack(tiles).astype(BF16)
            return carry
        lax.fori_loop(0, count // 2, body, 0)

    def forward_epilogue(pre, post):
        def epilogue(k, par, j, value):
            rounded = value.astype(BF16)
            pre[k, par] = rounded
            post[k, par] = with_edges(gelu_tanh(rounded.astype(F32))).astype(BF16) * img_mask[...]
        return epilogue

    def backward_epilogue(pre, post):
        def epilogue(k, par, j, value):
            slope = gelu_slope(pre[k, par].astype(F32))
            post[k, par] = with_edges(value * slope).astype(BF16) * img_mask[...]
        return epilogue

    core = lax.rem(row_id, 2)
    chip = col_id * 2 + row_id // 2
    n_chips = n_dev // 2
    partner = {'col': col_id, 'row': row_id + 1 - 2 * core}
    MESH = pl.DeviceIdType.MESH

    def pair_start(u):
        i, base, rows = UNITS[u]
        pltpu.make_async_remote_copy(
            src_ref=part.at[i, pl.ds(base + (1 - core) * (rows // 2), rows // 2)],
            dst_ref=pair_got.at[i, pl.ds(base // 2, rows // 2)],
            send_sem=sum_send.at[u, 0], recv_sem=sum_recv.at[u, 0], device_id=partner, device_id_type=MESH).start()

    def wait_half(u, sem):
        i, base, rows = UNITS[u]
        ref = half.at[i, pl.ds(base // 2, rows // 2)]
        pltpu.make_async_copy(ref, ref, sem).wait()

    def wait_chunks(u, sem):
        i, base, rows = UNITS[u]
        ref = got.at[i, :, pl.ds(base // 16, rows // 16)]
        pltpu.make_async_copy(ref, ref, sem).wait()

    def pair_add(u):
        i, base, rows = UNITS[u]
        wait_half(u, sum_recv.at[u, 0])
        there = pl.ds(base // 2, rows // 2)
        half[i, there] = part[i, pl.ds(base + core * (rows // 2), rows // 2)] + pair_got[i, there]

    def to_chips(make):
        def body(d, carry):
            other = lax.rem(chip + d, n_chips)
            make(d, other, {'col': other // 2, 'row': lax.rem(other, 2) * 2 + core}).start()
            return carry
        lax.fori_loop(1, n_chips, body, 0)

    def chunk_start(u):
        i, base, rows = UNITS[u]
        size = rows // 16
        to_chips(lambda d, other, ids: pltpu.make_async_remote_copy(
            src_ref=half.at[i, pl.ds(base // 2 + other * size, size)], dst_ref=got.at[i, d - 1, pl.ds(base // 16, size)],
            send_sem=sum_send.at[u, 1], recv_sem=sum_recv.at[u, 1], device_id=ids, device_id_type=MESH))

    def mine(u):
        i, base, rows = UNITS[u]
        return pl.ds(base + core * (rows // 2) + chip * (rows // 16), rows // 16)

    def chunk_add(u):
        i, base, rows = UNITS[u]
        size = rows // 16
        wait_chunks(u, sum_recv.at[u, 1])
        total = half[i, pl.ds(base // 2 + chip * size, size)]
        for d in range(n_chips - 1):
            total = total + got[i, d, base // 16:base // 16 + size]
        final[i, mine(u)] = total

    def spread_start(u):
        i = UNITS[u][0]
        to_chips(lambda d, other, ids: pltpu.make_async_remote_copy(
            src_ref=final.at[i, mine(u)], dst_ref=final.at[i, mine(u)],
            send_sem=sum_send.at[u, 2], recv_sem=sum_recv.at[u, 2], device_id=ids, device_id_type=MESH))

    def return_start(u):
        i, base, rows = UNITS[u]
        wait_chunks(u, sum_recv.at[u, 2])
        ref = final.at[i, pl.ds(base + core * (rows // 2), rows // 2)]
        pltpu.make_async_remote_copy(
            src_ref=ref, dst_ref=ref, send_sem=sum_send.at[u, 3], recv_sem=sum_recv.at[u, 3],
            device_id=partner, device_id_type=MESH).start()

    def return_wait(u):
        wait_half(u, sum_recv.at[u, 3])

    local(0).wait()
    halo_do(0, over, 0, 'recv')
    to_strips(0, d_one, xp, 1, 0, 2)
    first_step = forward_epilogue(a_one, one)

    def first_body(c, carry):
        halo_do(0, sides, c, 'recv')
        to_strips(0, d_one, xp, 1, 2 + c * 16, 16)

        @pl.when((c == 0) & (row_id == 0))
        def _():
            xp[1:3] = jnp.zeros((2, 2, PAD_STEPS, STRIPS, CH), BF16)
        conv_stage(xp, 1, wp.at[0], c * 16, 16, 16, first_step)
        return carry
    lax.fori_loop(0, SIDES, first_body, 0)
    halo_do(0, under, 0, 'recv')
    halo_start(1)
    to_strips(0, d_one, xp, 1, PAIRS - 2, 2)
    mask_rows(xp, 1)
    conv_stage(xp, 1, wp.at[0], 64, 4, 4, first_step)
    mask_rows(one)
    conv_stage(one, 0, wp.at[1], 1, PAIRS - 2, 22, forward_epilogue(a_two, two))
    mask_rows(two)
    local(1).wait()
    halo_do(1, over, 0, 'recv')
    for chunk in range(SIDES):
        halo_do(1, sides, chunk, 'recv')
    halo_do(1, under, 0, 'recv')
    to_strips(1, d_two, gp, 0, 0, PAIRS)
    mask_rows(gp)
    d_two[0, 1] = zero_row
    d_two[PAIRS - 1, 0] = zero_row
    conv_stage(gp, 0, wp.at[3], 1, PAIRS - 2, 22, backward_epilogue(a_two, d_two))
    mask_rows(d_two)

    def call(fn, i):
        return lambda: fn(i)

    wgrad_stage(two, 0, gp, own_mask, acc, part.at[2], 16)
    pair_start(2)
    wgrad_stage(one, 0, d_two, own_mask, acc, part.at[1], 16,
                [(1, call(pair_add, 2)), (1, call(chunk_start, 2))])
    pair_start(1)
    conv_stage(d_two, 0, wp.at[4], 1, PAIRS - 2, 22, backward_epilogue(a_one, d_one),
               [(0, call(pair_add, 1)), (0, call(chunk_start, 1)), (1, call(chunk_add, 2)), (1, call(spread_start, 2))])
    mask_rows(d_one)
    wgrad_stage(xp, 1, d_one, own_mask, acc, part.at[0], 16,
                [(2, call(chunk_add, 1)), (2, call(spread_start, 1))], do_last=False)
    pair_start(0)
    wgrad_stage(xp, 1, d_one, own_mask, acc, part.at[0], 32,
                [(0, call(return_start, 2)), (1, call(pair_add, 0)), (1, call(chunk_start, 0))], do_pair=False)
    pair_start(3)

    def final_epilogue(skip, off, post):
        def epilogue(k, par, j, value):
            post[k, par] = (value + skip[k + off, par, 1:1 + STEPS].astype(F32)).astype(BF16)
        return epilogue

    conv_stage(two, 0, wp.at[2], FIRST_OWN, OWN_PAIRS, 16, final_epilogue(xp, 1, a_one),
               [(0, call(pair_add, 3)), (0, call(chunk_start, 3)), (2, call(return_start, 1)), (2, call(chunk_add, 0)),
                (2, call(spread_start, 0)), (3, call(chunk_add, 3)), (3, call(spread_start, 3))])
    conv_stage(d_one, 0, wp.at[5], FIRST_OWN, OWN_PAIRS, 16, final_epilogue(gp, 0, a_two),
               [(2, call(return_start, 0)), (2, call(return_start, 3))])
    for u in range(len(UNITS)):
        return_wait(u)
        wait_half(u, sum_send.at[u, 0])
        wait_chunks(u, sum_send.at[u, 1])
        wait_chunks(u, sum_send.at[u, 2])
        wait_half(u, sum_send.at[u, 3])
    for i in range(2):
        halo_do(i, over, 0, 'send')
        for chunk in range(SIDES):
            halo_do(i, sides, chunk, 'send')
        halo_do(i, under, 0, 'send')


def hand_over_kernel(y_strips, dx_strips, sums, block_out, grad_image, dw_first, dw_second, dw_third,
                     wide, lines, sems, dw_sems):
    dw_copies = [
        pltpu.make_async_copy(sums.at[i, pl.ds((q * 3 + p) * CH, CH)], dw.at[pl.ds((p * 3 + q) * CH, CH)], dw_sems.at[i, p * 3 + q])
        for i, dw in enumerate((dw_first, dw_second, dw_third)) for p in range(3) for q in range(3)]
    for copy in dw_copies:
        copy.start()

    for a, (strips, dst) in enumerate(((y_strips, block_out), (dx_strips, grad_image))):
        def store(b):
            return pltpu.make_async_copy(lines.at[a, b], dst.at[pl.ds(b * OUT_ROWS, OUT_ROWS)], sems.at[a, b])

        def body(b, carry):
            for r in range(OUT_ROWS):
                k, par = FIRST_OWN + b * (OUT_ROWS // 2) + r // 2, r % 2
                for t in range(STEPS):
                    wide[r, pl.ds(8 + t, STRIPS, stride=STEPS)] = strips[k, par, t].astype(F32)
            for r in range(OUT_ROWS):
                lines[a, b, r] = wide[r, 8 + COL_HALO:8 + COL_HALO + TILE].astype(BF16)
            store(b).start()
            return carry
        lax.fori_loop(0, TILE // OUT_ROWS, body, 0)

    for a, dst in enumerate((block_out, grad_image)):
        for b in range(TILE // OUT_ROWS):
            pltpu.make_async_copy(lines.at[a, b], dst.at[pl.ds(b * OUT_ROWS, OUT_ROWS)], sems.at[a, b]).wait()
    for copy in dw_copies:
        copy.wait()


def solution(mesh):
    assert (mesh.shape['row'], mesh.shape['col']) == (N_ROWS, N_COLS)
    act_spec = P(None, 'row', 'col', None)
    padded = (PAIRS, 2, PAD_STEPS, STRIPS, CH)
    plain = (PAIRS, 2, STEPS, STRIPS, CH)
    tile_shape = jax.ShapeDtypeStruct((TILE, TILE, CH), BF16)
    dw_shape = jax.ShapeDtypeStruct((9 * CH, CH), F32)
    hbm = pl.BlockSpec(memory_space=pl.ANY)
    vmem = pl.BlockSpec(memory_space=pltpu.VMEM)
    n_dev = N_ROWS * N_COLS
    call = pl.pallas_call(
        block_kernel,
        out_shape=(pltpu.VMEM(plain, BF16), pltpu.VMEM(plain, BF16), pltpu.VMEM((3, 9 * CH, CH), F32)),
        in_specs=[hbm] * 6 + [vmem] * 3,
        out_specs=(vmem,) * 3,
        scratch_shapes=[
            pltpu.VMEM((PAIRS + 2, 2, PAD_STEPS, STRIPS, CH), BF16),
            pltpu.VMEM(padded, BF16), pltpu.VMEM(padded, BF16), pltpu.VMEM(padded, BF16),
            pltpu.VMEM(padded, BF16), pltpu.VMEM(padded, BF16),
            pltpu.VMEM((6, 12 * CH, 2 * CH), BF16),
            pltpu.VMEM((2, 2, EXT_ROWS, QUAD, CH), BF16),
            pltpu.VMEM((16, EXT_COLS + 16, CH), F32),
            pltpu.VMEM((3 * CH, 3 * CH), F32),
            pltpu.VMEM((PAD_STEPS, STRIPS, CH), BF16),
            pltpu.VMEM((PAD_STEPS, STRIPS, CH), BF16),
            pltpu.VMEM((3, 9 * CH, CH), F32),
            pltpu.VMEM((3, HALF, CH), F32),
            pltpu.VMEM((3, HALF, CH), F32),
            pltpu.VMEM((3, n_dev // 2 - 1, CHUNK, CH), F32),
            pltpu.SemaphoreType.DMA((2,)),
            pltpu.SemaphoreType.DMA((2, 8, SIDES)),
            pltpu.SemaphoreType.DMA((2, 8, SIDES)),
            pltpu.SemaphoreType.DMA((len(UNITS), 4)),
            pltpu.SemaphoreType.DMA((len(UNITS), 4)),
        ],
        compiler_params=pltpu.CompilerParams(vmem_limit_bytes=54500000, collective_id=0, has_side_effects=True),
        name='block',
    )

    hand_over = pl.pallas_call(
        hand_over_kernel,
        out_shape=(tile_shape, tile_shape, dw_shape, dw_shape, dw_shape),
        in_specs=[vmem] * 3,
        out_specs=(hbm,) * 5,
        scratch_shapes=[
            pltpu.VMEM((OUT_ROWS, EXT_COLS + 16, CH), F32),
            pltpu.VMEM((2, TILE // OUT_ROWS, OUT_ROWS, TILE, CH), BF16),
            pltpu.SemaphoreType.DMA((2, TILE // OUT_ROWS)),
            pltpu.SemaphoreType.DMA((3, 9)),
        ],
        compiler_params=pltpu.CompilerParams(vmem_limit_bytes=32 * 2**20),
        name='hand_over',
    )

    def local_block(image, w_first, w_second, w_third, grad_out):
        views = []
        for tile in (image, grad_out):
            views += [tile.reshape(TILE, TILE, CH), tile.reshape(TILE, TILE // QUAD, QUAD, CH), tile.reshape(OWN_PAIRS, 2, TILE // STRIPS, STRIPS, CH)]
        out, dx, dw1, dw2, dw3 = hand_over(*call(*views, w_first, w_second, w_third))
        shape = (3, 3, CH, CH)
        return out[None], dx[None], dw1.reshape(shape), dw2.reshape(shape), dw3.reshape(shape)

    return jax.shard_map(local_block, mesh=mesh, in_specs=(act_spec, P(), P(), P(), act_spec), out_specs=(act_spec, act_spec, P(), P(), P()), check_vma=False)
```

```python
import functools
import math
import jax
import jax.numpy as jnp
from jax import lax
from jax.experimental import pallas as pl
from jax.experimental.pallas import tpu as pltpu
from jax.sharding import PartitionSpec as P

GELU_SCALE = math.sqrt(2.0 / math.pi)
GELU_CUBIC = 0.044715
BF16 = jnp.bfloat16
F32 = jnp.float32

TILE = 128
CH = 128
ROW_HALO = 4
COL_HALO = 8
STRIPS = 16
STEPS = 9
PAD_STEPS = STEPS + 2
PAIRS = 68
FIRST_OWN = ROW_HALO // 2
OWN_PAIRS = TILE // 2
EXT_ROWS = TILE + 2 * ROW_HALO
EXT_COLS = TILE + 2 * COL_HALO
QUAD = 4
N_ROWS = 4
N_COLS = 4
UNITS = ((0, 0, 6 * CH), (1, 0, 9 * CH), (2, 0, 9 * CH), (0, 6 * CH, 3 * CH))
OUT_ROWS = 16
SIDES = 4
SIDE_ROWS = TILE // SIDES
HALF = 9 * CH // 2
CHUNK = 9 * CH // (N_ROWS * N_COLS)


def gelu_arg(value, square):
    return jnp.tanh(value * (GELU_SCALE + (GELU_SCALE * GELU_CUBIC) * square))


def gelu_tanh(value):
    return 0.5 * value * (1.0 + gelu_arg(value, value * value))


def gelu_slope(value):
    square = value * value
    s = 0.5 + 0.5 * gelu_arg(value, square)
    return s + (s * (1.0 - s) * value) * (2.0 * GELU_SCALE + (6.0 * GELU_SCALE * GELU_CUBIC) * square)


def row_at(ref, k, r, off):
    pair = k - 1 if r == 0 else k + 1 if r == 3 else k
    return pair + off, (r + 1) % 2


def pack_weights(w_ref, wp_ref, back):
    zero = jnp.zeros((CH, CH), BF16)
    for q in range(3):
        for p in range(3):
            if back:
                block = w_ref[2 - p, 2 - q].astype(F32).T.astype(BF16)
            else:
                block = w_ref[p, q]
            for b in range(2):
                wp_ref[pl.ds((q * 4 + p + b) * CH, CH), pl.ds(b * CH, CH)] = block
        wp_ref[pl.ds((q * 4 + 3) * CH, CH), pl.ds(0, CH)] = zero
        wp_ref[pl.ds((q * 4) * CH, CH), pl.ds(CH, CH)] = zero


def run_hooks(hooks, step):
    for at, hook in hooks:
        @pl.when(step == at)
        def _():
            hook()


def conv_stage(src, off, wp, first, count, per_step, epilogue, hooks=()):
    def body(step, carry):
        base = first + step * per_step
        for j in range(per_step):
            k = base + j
            parts = []
            for q in range(3):
                for r in range(4):
                    pair, par = row_at(src, k, r, off)
                    parts.append(src[pair, par, q:q + STEPS].reshape(STEPS * STRIPS, CH))
            acc = jnp.dot(jnp.concatenate(parts, axis=1), wp[...], preferred_element_type=F32)
            for par in range(2):
                epilogue(k, par, j, acc[:, par * CH:(par + 1) * CH].reshape(STEPS, STRIPS, CH))
        run_hooks(hooks, step)
        return carry
    lax.fori_loop(0, count // per_step, body, 0)


def with_edges(value):
    left = pltpu.roll(value[STEPS - 1], 1, 0)[None]
    right = pltpu.roll(value[0], STRIPS - 1, 0)[None]
    return jnp.concatenate([left, value, right], axis=0)


def wgrad_stage(val, off, grad, own_mask, acc, out, per_step, hooks=(), do_pair=True, do_last=True):
    dims = (((0,), (0,)), ((), ()))
    flat = per_step * STEPS * STRIPS
    acc[...] = jnp.zeros_like(acc)

    def rows_of(k, r):
        pair, par = row_at(val, k, r, off)
        return val[pl.ds(pair, per_step), par, 1:1 + STEPS].reshape(flat, CH)

    def body(step, carry):
        k = FIRST_OWN + step * per_step
        rows = [rows_of(k, r) for r in range(4)]
        shifted = []
        for par in range(2):
            d = grad[pl.ds(k, per_step), par] * own_mask[...][None]
            shifted.append([d[:, 2 - q:2 - q + STEPS].reshape(flat, CH) for q in range(3)])
        if do_pair:
            lhs = jnp.concatenate([jnp.concatenate(rows[par:par + 3], axis=1) for par in range(2)], axis=0)
            rhs = jnp.concatenate([jnp.concatenate(shifted[par][:2], axis=1) for par in range(2)], axis=0)
            acc[:, 0:2 * CH] += lax.dot_general(lhs, rhs, dims, preferred_element_type=F32)
        if do_last:
            both = jnp.concatenate([shifted[0][2], shifted[1][2]], axis=1)
            last = lax.dot_general(jnp.concatenate(rows, axis=1), both, dims, preferred_element_type=F32)
            acc[:, 2 * CH:3 * CH] += last[0:3 * CH, 0:CH] + last[CH:4 * CH, CH:2 * CH]
        run_hooks(hooks, step)
        return carry

    lax.fori_loop(0, OWN_PAIRS // per_step, body, 0)
    for q in ([0, 1] if do_pair else []) + ([2] if do_last else []):
        out[q * 3 * CH:(q + 1) * 3 * CH] = acc[:, q * CH:(q + 1) * CH]


def directions():
    return [(dr, dc) for dr in (-1, 0, 1) for dc in (-1, 0, 1) if (dr, dc) != (0, 0)]


def block_kernel(image, image_quads, image_pairs, grad, grad_quads, grad_pairs, w_first, w_second, w_third,
                 a_one, a_two, final,
                 xp, one, two, gp, d_two, d_one, wp,
                 halo, wide, acc, img_mask, own_mask, part, pair_got, half, got,
                 in_sems, halo_send, halo_recv, sum_send, sum_recv):
    n_rows, n_cols = N_ROWS, N_COLS
    n_dev = n_rows * n_cols
    row_id = lax.axis_index('row')
    col_id = lax.axis_index('col')
    me = col_id * n_rows + row_id

    def local(i):
        src, dst = ((image_pairs, d_one), (grad_pairs, d_two))[i]
        return pltpu.make_async_copy(src, dst.at[pl.ds(FIRST_OWN, OWN_PAIRS), :, pl.ds(0, 8)], in_sems.at[i])

    local(0).start()
    local(1).start()

    barrier = pltpu.get_barrier_semaphore()

    def device(d):
        other = lax.rem(me + d, n_dev)
        return other, {'col': other // n_rows, 'row': lax.rem(other, n_rows)}

    def greet(d, carry):
        pl.semaphore_signal(barrier, inc=1, device_id=device(d)[1], device_id_type=pl.DeviceIdType.MESH)
        return carry
    lax.fori_loop(1, n_dev, greet, 0)

    strip = lax.broadcasted_iota(jnp.int32, (PAD_STEPS, STRIPS, CH), 1)
    step = lax.broadcasted_iota(jnp.int32, (PAD_STEPS, STRIPS, CH), 0) - 1
    column = strip * STEPS + step
    own = (column >= COL_HALO) & (column < COL_HALO + TILE)
    own_mask[...] = own.astype(F32).astype(BF16)
    lowest = jnp.where(col_id == 0, COL_HALO, -1)
    highest = jnp.where(col_id == n_cols - 1, COL_HALO + TILE, EXT_COLS + 1)
    img_mask[...] = ((column >= lowest) & (column < highest)).astype(F32).astype(BF16)
    zero_row = jnp.zeros((PAD_STEPS, STRIPS, CH), BF16)
    xp[0, 1] = zero_row
    xp[PAIRS + 1, 0] = zero_row
    wide[:, 0:16] = jnp.zeros((16, 16, CH), F32)
    wide[:, TILE + 16:TILE + 32] = jnp.zeros((16, 16, CH), F32)

    @pl.when(col_id == 0)
    def _():
        halo[0, 0] = jnp.zeros((EXT_ROWS, QUAD, CH), BF16)
        halo[1, 0] = jnp.zeros((EXT_ROWS, QUAD, CH), BF16)

    @pl.when(col_id == n_cols - 1)
    def _():
        halo[0, 1] = jnp.zeros((EXT_ROWS, QUAD, CH), BF16)
        halo[1, 1] = jnp.zeros((EXT_ROWS, QUAD, CH), BF16)

    pl.semaphore_wait(barrier, n_dev - 1)

    def halo_copy(i, n, dr, dc, chunk=0):
        quads, pairs, natural = ((image_quads, image_pairs, d_one), (grad_quads, grad_pairs, d_two))[i]
        if dc == 0:
            src = pairs.at[pl.ds(0, 2)] if dr < 0 else pairs.at[pl.ds(OWN_PAIRS - 2, 2)]
            dst = natural.at[pl.ds(PAIRS - 2, 2) if dr < 0 else pl.ds(0, 2), :, pl.ds(0, 8)]
        else:
            side = pl.ds(chunk * SIDE_ROWS, SIDE_ROWS)
            rows = (pl.ds(0, ROW_HALO), side, pl.ds(TILE - ROW_HALO, ROW_HALO))[dr + 1]
            into = (pl.ds(EXT_ROWS - ROW_HALO, ROW_HALO), pl.ds(ROW_HALO + chunk * SIDE_ROWS, SIDE_ROWS), pl.ds(0, ROW_HALO))[dr + 1]
            src = quads.at[rows, 0 if dc < 0 else TILE // QUAD - 1]
            dst = halo.at[i, 1 if dc < 0 else 0, into]
        return pltpu.make_async_remote_copy(
            src_ref=src, dst_ref=dst, send_sem=halo_send.at[i, n, chunk], recv_sem=halo_recv.at[i, n, chunk],
            device_id={'col': col_id + dc, 'row': row_id + dr}, device_id_type=pl.DeviceIdType.MESH)

    def exists(dr, dc):
        ok = None
        for pos, shift, size in ((row_id, dr, n_rows), (col_id, dc, n_cols)):
            if shift:
                one_ok = (pos + shift >= 0) & (pos + shift < size)
                ok = one_ok if ok is None else ok & one_ok
        return ok

    around = list(enumerate(directions()))
    sides = [(n, d) for n, d in around if d[0] == 0]
    over = [(n, d) for n, d in around if d[0] == 1]
    under = [(n, d) for n, d in around if d[0] == -1]

    def halo_do(i, group, chunk, what):
        for n, (dr, dc) in group:
            flip = -1 if what == 'recv' else 1

            @pl.when(exists(flip * dr, flip * dc))
            def _():
                copy = halo_copy(i, n, dr, dc, chunk)
                if what == 'start':
                    copy.start()
                elif what == 'recv':
                    copy.wait_recv()
                else:
                    copy.wait_send()

    def halo_start(i):
        halo_do(i, sides, 0, 'start')
        halo_do(i, over, 0, 'start')
        for chunk in range(1, SIDES):
            halo_do(i, sides, chunk, 'start')
        halo_do(i, under, 0, 'start')

    halo_start(0)

    for i, (w_ref, back) in enumerate(((w_first, False), (w_second, False), (w_third, False), (w_third, True), (w_second, True), (w_first, True))):
        pack_weights(w_ref, wp.at[i], back)

    def mask_rows(ref, off=0):
        zeros = jnp.zeros((2, 2, PAD_STEPS, STRIPS, CH), BF16)

        @pl.when(row_id == 0)
        def _():
            ref[off:off + 2] = zeros

        @pl.when(row_id == n_rows - 1)
        def _():
            ref[off + PAIRS - 2:off + PAIRS] = zeros

    def to_strips(i, natural, dst, off, first, count):
        def body(b, carry):
            for r in range(4):
                k, par = first + 2 * b + r // 2, r % 2
                wide[r, 16:16 + TILE] = natural[k, par, 0:8].reshape(TILE, CH).astype(F32)
                wide[r, 16 - QUAD:16] = halo[i, 0, 2 * k + par].astype(F32)
                wide[r, 16 + TILE:16 + TILE + QUAD] = halo[i, 1, 2 * k + par].astype(F32)
            for r in range(4):
                k, par = first + 2 * b + r // 2, r % 2
                tiles = [wide[r, pl.ds(7 + t, STRIPS, stride=STEPS)] for t in range(PAD_STEPS)]
                dst[off + k, par] = jnp.stack(tiles).astype(BF16)
            return carry
        lax.fori_loop(0, count // 2, body, 0)

    def forward_epilogue(pre, post):
        def epilogue(k, par, j, value):
            rounded = value.astype(BF16)
            pre[k, par] = rounded
            post[k, par] = with_edges(gelu_tanh(rounded.astype(F32))).astype(BF16) * img_mask[...]
        return epilogue

    def backward_epilogue(pre, post):
        def epilogue(k, par, j, value):
            slope = gelu_slope(pre[k, par].astype(F32))
            post[k, par] = with_edges(value * slope).astype(BF16) * img_mask[...]
        return epilogue

    core = lax.rem(row_id, 2)
    chip = col_id * 2 + row_id // 2
    n_chips = n_dev // 2
    partner = {'col': col_id, 'row': row_id + 1 - 2 * core}
    MESH = pl.DeviceIdType.MESH

    def pair_start(u):
        i, base, rows = UNITS[u]
        pltpu.make_async_remote_copy(
            src_ref=part.at[i, pl.ds(base + (1 - core) * (rows // 2), rows // 2)],
            dst_ref=pair_got.at[i, pl.ds(base // 2, rows // 2)],
            send_sem=sum_send.at[u, 0], recv_sem=sum_recv.at[u, 0], device_id=partner, device_id_type=MESH).start()

    def wait_half(u, sem):
        i, base, rows = UNITS[u]
        ref = half.at[i, pl.ds(base // 2, rows // 2)]
        pltpu.make_async_copy(ref, ref, sem).wait()

    def wait_chunks(u, sem):
        i, base, rows = UNITS[u]
        ref = got.at[i, :, pl.ds(base // 16, rows // 16)]
        pltpu.make_async_copy(ref, ref, sem).wait()

    def pair_add(u):
        i, base, rows = UNITS[u]
        wait_half(u, sum_recv.at[u, 0])
        there = pl.ds(base // 2, rows // 2)
        half[i, there] = part[i, pl.ds(base + core * (rows // 2), rows // 2)] + pair_got[i, there]

    def to_chips(make):
        def body(d, carry):
            other = lax.rem(chip + d, n_chips)
            make(d, other, {'col': other // 2, 'row': lax.rem(other, 2) * 2 + core}).start()
            return carry
        lax.fori_loop(1, n_chips, body, 0)

    def chunk_start(u):
        i, base, rows = UNITS[u]
        size = rows // 16
        to_chips(lambda d, other, ids: pltpu.make_async_remote_copy(
            src_ref=half.at[i, pl.ds(base // 2 + other * size, size)], dst_ref=got.at[i, d - 1, pl.ds(base // 16, size)],
            send_sem=sum_send.at[u, 1], recv_sem=sum_recv.at[u, 1], device_id=ids, device_id_type=MESH))

    def mine(u):
        i, base, rows = UNITS[u]
        return pl.ds(base + core * (rows // 2) + chip * (rows // 16), rows // 16)

    def chunk_add(u):
        i, base, rows = UNITS[u]
        size = rows // 16
        wait_chunks(u, sum_recv.at[u, 1])
        total = half[i, pl.ds(base // 2 + chip * size, size)]
        for d in range(n_chips - 1):
            total = total + got[i, d, base // 16:base // 16 + size]
        final[i, mine(u)] = total

    def spread_start(u):
        i = UNITS[u][0]
        to_chips(lambda d, other, ids: pltpu.make_async_remote_copy(
            src_ref=final.at[i, mine(u)], dst_ref=final.at[i, mine(u)],
            send_sem=sum_send.at[u, 2], recv_sem=sum_recv.at[u, 2], device_id=ids, device_id_type=MESH))

    def return_start(u):
        i, base, rows = UNITS[u]
        wait_chunks(u, sum_recv.at[u, 2])
        ref = final.at[i, pl.ds(base + core * (rows // 2), rows // 2)]
        pltpu.make_async_remote_copy(
            src_ref=ref, dst_ref=ref, send_sem=sum_send.at[u, 3], recv_sem=sum_recv.at[u, 3],
            device_id=partner, device_id_type=MESH).start()

    def return_wait(u):
        wait_half(u, sum_recv.at[u, 3])

    local(0).wait()
    halo_do(0, over, 0, 'recv')
    to_strips(0, d_one, xp, 1, 0, 2)
    first_step = forward_epilogue(a_one, one)

    def first_body(c, carry):
        halo_do(0, sides, c, 'recv')
        to_strips(0, d_one, xp, 1, 2 + c * 16, 16)

        @pl.when((c == 0) & (row_id == 0))
        def _():
            xp[1:3] = jnp.zeros((2, 2, PAD_STEPS, STRIPS, CH), BF16)
        conv_stage(xp, 1, wp.at[0], c * 16, 16, 16, first_step)
        return carry
    lax.fori_loop(0, SIDES, first_body, 0)
    halo_do(0, under, 0, 'recv')
    halo_start(1)
    to_strips(0, d_one, xp, 1, PAIRS - 2, 2)
    mask_rows(xp, 1)
    conv_stage(xp, 1, wp.at[0], 64, 4, 4, first_step)
    mask_rows(one)
    conv_stage(one, 0, wp.at[1], 1, PAIRS - 2, 22, forward_epilogue(a_two, two))
    mask_rows(two)
    local(1).wait()
    halo_do(1, over, 0, 'recv')
    for chunk in range(SIDES):
        halo_do(1, sides, chunk, 'recv')
    halo_do(1, under, 0, 'recv')
    to_strips(1, d_two, gp, 0, 0, PAIRS)
    mask_rows(gp)
    d_two[0, 1] = zero_row
    d_two[PAIRS - 1, 0] = zero_row
    conv_stage(gp, 0, wp.at[3], 1, PAIRS - 2, 22, backward_epilogue(a_two, d_two))
    mask_rows(d_two)

    def call(fn, i):
        return lambda: fn(i)

    wgrad_stage(two, 0, gp, own_mask, acc, part.at[2], 32)
    pair_start(2)
    wgrad_stage(one, 0, d_two, own_mask, acc, part.at[1], 32,
                [(0, call(pair_add, 2)), (0, call(chunk_start, 2))])
    pair_start(1)
    conv_stage(d_two, 0, wp.at[4], 1, PAIRS - 2, 22, backward_epilogue(a_one, d_one),
               [(0, call(pair_add, 1)), (0, call(chunk_start, 1)), (1, call(chunk_add, 2)), (1, call(spread_start, 2))])
    mask_rows(d_one)
    wgrad_stage(xp, 1, d_one, own_mask, acc, part.at[0], 16,
                [(2, call(chunk_add, 1)), (2, call(spread_start, 1))], do_last=False)
    pair_start(0)
    wgrad_stage(xp, 1, d_one, own_mask, acc, part.at[0], 32,
                [(0, call(return_start, 2)), (1, call(pair_add, 0)), (1, call(chunk_start, 0))], do_pair=False)
    pair_start(3)

    def final_epilogue(skip, off, post):
        def epilogue(k, par, j, value):
            post[k, par] = (value + skip[k + off, par, 1:1 + STEPS].astype(F32)).astype(BF16)
        return epilogue

    conv_stage(two, 0, wp.at[2], FIRST_OWN, OWN_PAIRS, 16, final_epilogue(xp, 1, a_one),
               [(0, call(pair_add, 3)), (0, call(chunk_start, 3)), (2, call(return_start, 1)), (2, call(chunk_add, 0)),
                (2, call(spread_start, 0)), (3, call(chunk_add, 3)), (3, call(spread_start, 3))])
    conv_stage(d_one, 0, wp.at[5], FIRST_OWN, OWN_PAIRS, 16, final_epilogue(gp, 0, a_two),
               [(2, call(return_start, 0)), (2, call(return_start, 3))])
    for u in range(len(UNITS)):
        return_wait(u)
        wait_half(u, sum_send.at[u, 0])
        wait_chunks(u, sum_send.at[u, 1])
        wait_chunks(u, sum_send.at[u, 2])
        wait_half(u, sum_send.at[u, 3])
    for i in range(2):
        halo_do(i, over, 0, 'send')
        for chunk in range(SIDES):
            halo_do(i, sides, chunk, 'send')
        halo_do(i, under, 0, 'send')


def hand_over_kernel(y_strips, dx_strips, sums, block_out, grad_image, dw_first, dw_second, dw_third,
                     wide, lines, sems, dw_sems):
    dw_copies = [
        pltpu.make_async_copy(sums.at[i, pl.ds((q * 3 + p) * CH, CH)], dw.at[pl.ds((p * 3 + q) * CH, CH)], dw_sems.at[i, p * 3 + q])
        for i, dw in enumerate((dw_first, dw_second, dw_third)) for p in range(3) for q in range(3)]
    for copy in dw_copies:
        copy.start()

    for a, (strips, dst) in enumerate(((y_strips, block_out), (dx_strips, grad_image))):
        def store(b):
            return pltpu.make_async_copy(lines.at[a, b], dst.at[pl.ds(b * OUT_ROWS, OUT_ROWS)], sems.at[a, b])

        def body(b, carry):
            for r in range(OUT_ROWS):
                k, par = FIRST_OWN + b * (OUT_ROWS // 2) + r // 2, r % 2
                for t in range(STEPS):
                    wide[r, pl.ds(8 + t, STRIPS, stride=STEPS)] = strips[k, par, t].astype(F32)
            for r in range(OUT_ROWS):
                lines[a, b, r] = wide[r, 8 + COL_HALO:8 + COL_HALO + TILE].astype(BF16)
            store(b).start()
            return carry
        lax.fori_loop(0, TILE // OUT_ROWS, body, 0)

    for a, dst in enumerate((block_out, grad_image)):
        for b in range(TILE // OUT_ROWS):
            pltpu.make_async_copy(lines.at[a, b], dst.at[pl.ds(b * OUT_ROWS, OUT_ROWS)], sems.at[a, b]).wait()
    for copy in dw_copies:
        copy.wait()


def solution(mesh):
    assert (mesh.shape['row'], mesh.shape['col']) == (N_ROWS, N_COLS)
    act_spec = P(None, 'row', 'col', None)
    padded = (PAIRS, 2, PAD_STEPS, STRIPS, CH)
    plain = (PAIRS, 2, STEPS, STRIPS, CH)
    tile_shape = jax.ShapeDtypeStruct((TILE, TILE, CH), BF16)
    dw_shape = jax.ShapeDtypeStruct((9 * CH, CH), F32)
    hbm = pl.BlockSpec(memory_space=pl.ANY)
    vmem = pl.BlockSpec(memory_space=pltpu.VMEM)
    n_dev = N_ROWS * N_COLS
    call = pl.pallas_call(
        block_kernel,
        out_shape=(pltpu.VMEM(plain, BF16), pltpu.VMEM(plain, BF16), pltpu.VMEM((3, 9 * CH, CH), F32)),
        in_specs=[hbm] * 6 + [vmem] * 3,
        out_specs=(vmem,) * 3,
        scratch_shapes=[
            pltpu.VMEM((PAIRS + 2, 2, PAD_STEPS, STRIPS, CH), BF16),
            pltpu.VMEM(padded, BF16), pltpu.VMEM(padded, BF16), pltpu.VMEM(padded, BF16),
            pltpu.VMEM(padded, BF16), pltpu.VMEM(padded, BF16),
            pltpu.VMEM((6, 12 * CH, 2 * CH), BF16),
            pltpu.VMEM((2, 2, EXT_ROWS, QUAD, CH), BF16),
            pltpu.VMEM((16, EXT_COLS + 16, CH), F32),
            pltpu.VMEM((3 * CH, 3 * CH), F32),
            pltpu.VMEM((PAD_STEPS, STRIPS, CH), BF16),
            pltpu.VMEM((PAD_STEPS, STRIPS, CH), BF16),
            pltpu.VMEM((3, 9 * CH, CH), F32),
            pltpu.VMEM((3, HALF, CH), F32),
            pltpu.VMEM((3, HALF, CH), F32),
            pltpu.VMEM((3, n_dev // 2 - 1, CHUNK, CH), F32),
            pltpu.SemaphoreType.DMA((2,)),
            pltpu.SemaphoreType.DMA((2, 8, SIDES)),
            pltpu.SemaphoreType.DMA((2, 8, SIDES)),
            pltpu.SemaphoreType.DMA((len(UNITS), 4)),
            pltpu.SemaphoreType.DMA((len(UNITS), 4)),
        ],
        compiler_params=pltpu.CompilerParams(vmem_limit_bytes=54500000, collective_id=0, has_side_effects=True),
        name='block',
    )

    hand_over = pl.pallas_call(
        hand_over_kernel,
        out_shape=(tile_shape, tile_shape, dw_shape, dw_shape, dw_shape),
        in_specs=[vmem] * 3,
        out_specs=(hbm,) * 5,
        scratch_shapes=[
            pltpu.VMEM((OUT_ROWS, EXT_COLS + 16, CH), F32),
            pltpu.VMEM((2, TILE // OUT_ROWS, OUT_ROWS, TILE, CH), BF16),
            pltpu.SemaphoreType.DMA((2, TILE // OUT_ROWS)),
            pltpu.SemaphoreType.DMA((3, 9)),
        ],
        compiler_params=pltpu.CompilerParams(vmem_limit_bytes=32 * 2**20),
        name='hand_over',
    )

    def local_block(image, w_first, w_second, w_third, grad_out):
        views = []
        for tile in (image, grad_out):
            views += [tile.reshape(TILE, TILE, CH), tile.reshape(TILE, TILE // QUAD, QUAD, CH), tile.reshape(OWN_PAIRS, 2, TILE // STRIPS, STRIPS, CH)]
        out, dx, dw1, dw2, dw3 = hand_over(*call(*views, w_first, w_second, w_third))
        shape = (3, 3, CH, CH)
        return out[None], dx[None], dw1.reshape(shape), dw2.reshape(shape), dw3.reshape(shape)

    return jax.shard_map(local_block, mesh=mesh, in_specs=(act_spec, P(), P(), P(), act_spec), out_specs=(act_spec, act_spec, P(), P(), P()), check_vma=False)
```
